512 devices in a mesh: grp: 2 (over y_lo), zt: 16 (over x, y_hi), xy: 16 (over z, core).
Axes of the slice: x: 4, y: 8 (y_hi: 4, y_lo: 2; y = y_hi * 2 + y_lo), z: 8, core: 2. Of those that a mesh axis runs over, the one named last changes fastest.
Arguments:
- source: float32 [2, 2, 3, 32, 64, 128], P('grp', None, None, 'xy', 'zt'), may hold values from -6 to 6
- links: float32 [4, 2, 3, 3, 32, 64, 128], P('grp', None, None, None, 'xy', 'zt'), may hold values from -2 to 2
- shifts: float32 [12], replicated, may hold values from 0.01 to 0.5
- residues: float32 [12], replicated, may hold values from 0.05 to 0.5
- mass: float32 [1], replicated, may hold values from 0.1 to 0.5
Outputs:
- rational: float32 [2, 2, 3, 32, 64, 128], P('grp', None, None, 'xy', 'zt')
- action: float32 [1], replicated
The draws below stay inside these ranges and needn't reach their ends.
All inputs are finite; a program needn't handle non-finite values.
Results may differ from the reference program's by a relative error of at most 0.0003.
Values sent between devices are 32-bit elements; how exact they have to be, the bound alone decides.
No kernel may reach another device: no remote copies, remote signals or barrier semaphores. Data moves between devices by JAX's collectives and lax.ppermute only.
A program may use at most 64 MiB of HBM per device.

```python
import math
import jax
import jax.numpy as jnp

NY = 2
NZ = 64
NSHIFT = 12
ITERS = 8
PF = 2
NX = 32
NT = 64


def levels(own_key, extent, split, smallest, high):
    def one(position, shards_of):
        draws = jax.random.uniform(jax.random.fold_in(jax.random.fold_in(own_key, 6), position), (shards_of,), jnp.float32, smallest / len(split), high / len(split))
        return jnp.repeat(jnp.exp(draws), extent[position] // shards_of).reshape((-1,) + (1,) * (len(extent) - position - 1))

    gain = one(*split[0])
    for cut in split[1:]:
        gain = gain * one(*cut)
    return gain


def centred(own_key, dims, width, bound, cuts=(), held_as=jnp.bfloat16):
    result = width * jax.random.normal(own_key, dims, jnp.float32)
    if cuts:
        result = result * levels(own_key, dims, cuts, -0.22, 0.18)
    return jnp.clip(result, -bound, bound).astype(held_as)


def setup_inputs(seed: int = 0) -> dict:
    key_of = jax.random.split(jax.random.key(seed), 6)
    return {
        "source": centred(key_of[0], (PF, 2, 3, NX, NT, NY * NZ), 1.0, 6.0, ((0, 2), (3, 16), (4, 16)), jnp.float32),
        "links": centred(key_of[1], (4, 2, 3, 3, NX, NT, NY * NZ), 0.35, 2.0, ((0, 2), (4, 16), (5, 16)), jnp.float32),
        "shifts": jnp.clip(jnp.exp(jax.random.uniform(key_of[2], (NSHIFT,), jnp.float32, math.log(0.01), math.log(0.5))), 0.01, 0.5),
        "residues": jnp.clip(jnp.exp(jax.random.uniform(key_of[3], (NSHIFT,), jnp.float32, math.log(0.05), math.log(0.5))), 0.05, 0.5),
        "mass": jnp.clip(jnp.exp(jax.random.uniform(key_of[4], (1,), jnp.float32, math.log(0.1), math.log(0.5))), 0.1, 0.5),
    }


def sign_of(values):
    return (1 - 2 * (values % 2)).astype(jnp.float32)


def phases(coord_x, coord_t, last_t):
    yz_index = jnp.arange(NY * NZ, dtype=jnp.int32)
    ycoord = yz_index // NZ
    zcoord = yz_index % NZ
    unity = jnp.ones((coord_x.shape[0], coord_t.shape[0], NY * NZ), jnp.float32)
    boundary = jnp.where(coord_t == last_t, -1.0, 1.0).astype(jnp.float32)
    eta_y = sign_of(coord_x)[:, None, None] * unity
    eta_z = sign_of(coord_x[:, None, None] + ycoord[None, None, :]) * unity
    eta_t = sign_of(coord_x[:, None, None] + ycoord[None, None, :] + zcoord[None, None, :]) * boundary[None, :, None]
    return jnp.stack([unity, eta_y, eta_z, eta_t])


def times_link(link, field):
    real = jnp.sum(link[0][None] * field[:, 0][:, None] - link[1][None] * field[:, 1][:, None], axis=2)
    imag = jnp.sum(link[0][None] * field[:, 1][:, None] + link[1][None] * field[:, 0][:, None], axis=2)
    return jnp.stack([real, imag], axis=1)


def times_adjoint(link, field):
    real = jnp.sum(link[0][None] * field[:, 0][:, :, None] + link[1][None] * field[:, 1][:, :, None], axis=1)
    imag = jnp.sum(link[0][None] * field[:, 1][:, :, None] - link[1][None] * field[:, 0][:, :, None], axis=1)
    return jnp.stack([real, imag], axis=1)


def roll_ycoord(values, offset):
    return jnp.roll(values, offset * NZ, axis=-1)


def roll_zcoord(values, offset):
    shape = values.shape
    return jnp.roll(values.reshape(shape[:-1] + (NY, NZ)), offset, axis=-1).reshape(shape)


def hopping(field, folded):
    total = times_link(folded[0], jnp.roll(field, -1, axis=3)) - jnp.roll(times_adjoint(folded[0], field), 1, axis=3)
    total = total + times_link(folded[1], roll_ycoord(field, -1)) - roll_ycoord(times_adjoint(folded[1], field), 1)
    total = total + times_link(folded[2], roll_zcoord(field, -1)) - roll_zcoord(times_adjoint(folded[2], field), 1)
    total = total + times_link(folded[3], jnp.roll(field, -1, axis=4)) - jnp.roll(times_adjoint(folded[3], field), 1, axis=4)
    return 0.5 * total


def local_dot(left, right):
    return jnp.sum(left * right, axis=(1, 2, 3, 4, 5))


def spread(values):
    return values.reshape(values.shape + (1, 1, 1, 1, 1))


def rational_of(source, apply_normal, shifts, residues):
    shift_col = shifts[:, None]
    members = source.shape[0]
    residual = source
    direction = source
    solutions = jnp.zeros((shifts.shape[0],) + source.shape, jnp.float32)
    directions = jnp.broadcast_to(source[None], solutions.shape)
    norm_now = local_dot(source, source)
    zeta_now = jnp.ones((shifts.shape[0], members), jnp.float32)
    zeta_old = jnp.ones((shifts.shape[0], members), jnp.float32)
    alpha_old = jnp.ones((members,), jnp.float32)
    beta_old = jnp.zeros((members,), jnp.float32)
    for iteration in range(ITERS):
        image = apply_normal(direction)
        alpha_now = norm_now / local_dot(direction, image)
        zeta_new = zeta_now * zeta_old * alpha_old / (alpha_now * beta_old * (zeta_old - zeta_now) + zeta_old * alpha_old * (1.0 + shift_col * alpha_now))
        alpha_shift = alpha_now * zeta_new / zeta_now
        solutions = solutions + spread(alpha_shift) * directions
        if iteration + 1 < ITERS:
            residual = residual - spread(alpha_now) * image
            norm_next = local_dot(residual, residual)
            beta_now = norm_next / norm_now
            beta_shift = beta_now * (zeta_new / zeta_now) ** 2
            direction = residual + spread(beta_now) * direction
            directions = spread(zeta_new) * residual[None] + spread(beta_shift) * directions
            zeta_old = zeta_now
            zeta_now = zeta_new
            alpha_old = alpha_now
            beta_old = beta_now
            norm_now = norm_next
    return jnp.sum(residues.reshape((-1, 1, 1, 1, 1, 1, 1)) * solutions, axis=0)


def reference(source, links, shifts, residues, mass):
    eta = phases(jnp.arange(NX, dtype=jnp.int32), jnp.arange(NT, dtype=jnp.int32), NT - 1)
    folded = links * eta[:, None, None, None]
    mass_sq = mass[0] * mass[0]

    def apply_normal(field):
        return mass_sq * field - hopping(hopping(field, folded), folded)

    pieces = []
    for member in range(PF):
        pieces.append(rational_of(source[member:member + 1], apply_normal, shifts, residues))
    rational = jnp.concatenate(pieces, axis=0)
    action = (jnp.sum(source * rational) / (PF * NX * NT * NY * NZ)).reshape(1)
    return rational, action
```

```python
import functools

import jax
import jax.numpy as jnp
from jax import lax
from jax.experimental import pallas as pl
from jax.experimental.pallas import tpu as pltpu
from jax.sharding import Mesh
from jax.sharding import PartitionSpec as P

NY = 2
NZ = 64
LANES = NY * NZ
STEP = 4
XY = ("xy_0", "xy_1")
ZT = ("zt_0", "zt_1")
ZT_XY = ("zt_0", "zt_1", "xy_0", "xy_1")
F32 = jnp.float32
ROWS = 16
LX_N, L_N = 5, 4


def two_sum(a, b):
    s = a + b
    t = s - a
    return s, (a - (s - t)) + (b - t)


def quick_sum(a, b):
    s = a + b
    return s, b - (s - a)


def halves(a):
    t = a * 4097.0
    h = t - (t - a)
    return h, a - h


def two_prod(a, b):
    p = a * b
    ah, al = halves(a)
    bh, bl = halves(b)
    return p, ((ah * bh - p) + ah * bl + al * bh) + al * bl


@jax.tree_util.register_pytree_node_class
class Pair:
    def __init__(self, h, l):
        self.h = h
        self.l = l

    def tree_flatten(self):
        return (self.h, self.l), None

    @classmethod
    def tree_unflatten(cls, _, leaves):
        return cls(*leaves)

    def __add__(self, o):
        a, e = two_sum(self.h, o.h)
        t, f = two_sum(self.l, o.l)
        a, e = quick_sum(a, e + t)
        return Pair(*quick_sum(a, e + f))

    def __neg__(self):
        return Pair(-self.h, -self.l)

    def __sub__(self, o):
        return self + (-o)

    def __mul__(self, o):
        p, e = two_prod(self.h, o.h)
        return Pair(*quick_sum(p, e + (self.h * o.l + self.l * o.h)))

    def times(self, f):
        p, e = two_prod(self.h, f)
        return Pair(*quick_sum(p, e + self.l * f))

    def __truediv__(self, o):
        q1 = self.h / o.h
        r = self - o.times(q1)
        q2 = r.h / o.h
        r = r - o.times(q2)
        a, b = quick_sum(q1, q2)
        return Pair(*quick_sum(a, b + r.h / o.h))


def plus(a, b):
    return b if a is None else a + b


def run_steps(first, moments, state, m2, one, shifts, final):
    size = STEP
    al, be, c, gam = (dict(state[n]) for n in ("al", "be", "c", "gam"))
    coef = dict(state["coef"])
    part, sol = dict(state["part"]), dict(state["sol"])
    zeta, zeta_old, zeta_new = state["zeta"], state["zeta_old"], state["zeta_new"]
    unit = Pair(one, jnp.zeros_like(one))
    table = {first: list(moments)}
    raised = {}
    if first:
        inv, own, low = {}, {}, {}
        for k in range(first):
            inv[k] = unit / al[k]
            own[k] = (unit + c[k] if k else unit) * inv[k] - m2
            if k:
                low[k] = c[k] * inv[k]
            table[k] = [None] * (2 * size)
        for i in range(1, 2 * size):
            for k in range(first - 1, -1, -1):
                if i < first - k:
                    continue
                t = None
                if table[k][i - 1] is not None:
                    t = plus(t, own[k] * table[k][i - 1])
                if table[k + 1][i - 1] is not None:
                    t = plus(t, -(inv[k] * table[k + 1][i - 1]))
                if k and table[k - 1][i - 1] is not None:
                    t = plus(t, -(low[k] * table[k - 1][i - 1]))
                table[k][i] = t
        rest, top = state["handover"]
        scale = one / top
        for k in range(first - 1):
            raised[k] = {k + 1: one}
        raised[first - 1] = {j: -(rest[j] * scale) for j in rest}
        raised[first - 1][first] = scale
    for i in range(size - 1):
        raised[first + i] = {first + i + 1: one}
    coef[first] = {first: one}
    lead, second = unit, None
    handover = None
    for d in range(size):
        k = first + d
        norm = lead * table[k][d]
        high = lead * table[k][d + 1]
        if second is not None:
            high = high + second * table[k][d]
        gam[k] = norm
        if k == 0:
            part = {0: jnp.ones_like(shifts)}
        else:
            ratio = norm / gam[k - 1]
            be[k - 1] = ratio
            step = zeta_new / zeta
            keep = ratio.h * step * step
            grown = {}
            for j in sorted(set(part) | set(coef[k])):
                t = None
                if j in coef[k]:
                    t = zeta_new * coef[k][j]
                if j in part:
                    t = plus(t, keep * part[j])
                grown[j] = t
            part = grown
            zeta_old, zeta = zeta, zeta_new
        curve = m2 * norm + high
        if k:
            curve = curve - ratio * norm / al[k - 1]
        a = norm / curve
        al[k] = a
        if k:
            a_old, b_old = al[k - 1].h, be[k - 1].h
            zeta_new = (
                zeta
                * zeta_old
                * a_old
                / (a.h * b_old * (zeta_old - zeta) + zeta_old * a_old * (1.0 + shifts * a.h))
            )
            c[k] = a * be[k - 1] / al[k - 1]
            keep_r = unit + c[k]
        else:
            zeta_new = zeta / (1.0 + shifts * a.h)
            keep_r = unit
        gain = a.h * zeta_new / zeta
        for j in part:
            sol[j] = plus(sol.get(j), gain * part[j])
        if d == size - 1 and final:
            break
        image = {}
        for j, v in coef[k].items():
            image[j] = plus(image.get(j), m2.h * v)
            if j == first + size - 1:
                continue
            for jj, w in raised[j].items():
                image[jj] = plus(image.get(jj), w * v)
        following = {}
        for j in sorted(set(coef[k]) | set(image) | set(coef.get(k - 1, {}))):
            t = None
            if j in coef[k]:
                t = keep_r.h * coef[k][j]
            if j in image:
                t = plus(t, -(a.h * image[j]))
            if k and j in coef[k - 1]:
                t = plus(t, -(c[k].h * coef[k - 1][j]))
            following[j] = t
        if d == size - 1:
            handover = (following, -(a.h * coef[k][first + size - 1]))
            break
        coef[k + 1] = following
        row = [None] * (2 * size)
        for i in range(2 * size - 1 - d):
            if table[k][i] is None or table[k][i + 1] is None:
                continue
            t = keep_r * table[k][i] - a * (m2 * table[k][i] + table[k][i + 1])
            if k and table[k - 1][i] is not None:
                t = t - c[k] * table[k - 1][i]
            row[i] = t
        table[k + 1] = row
        image_second = m2 * lead if second is None else m2 * lead + second
        lead, second = -(a * lead), keep_r * lead - a * image_second
    last = first + size - 1
    return {
        "al": al,
        "be": be,
        "c": c,
        "gam": {last: gam[last]},
        "coef": {last: coef[last]},
        "part": part,
        "sol": sol,
        "zeta": zeta,
        "zeta_old": zeta_old,
        "zeta_new": zeta_new,
        "handover": handover,
    }


def start_state(one):
    return {
        "al": {},
        "be": {},
        "c": {},
        "gam": {},
        "coef": {},
        "part": {},
        "sol": {},
        "zeta": one,
        "zeta_old": one,
        "zeta_new": one,
        "handover": None,
    }


def first_state(moments, m2, shifts):
    one = jnp.ones_like(shifts)
    return run_steps(0, moments, start_state(one), m2, one, shifts, False)


def state_shape():
    s = jax.ShapeDtypeStruct((8, LANES), F32)
    moments = [Pair(s, s)] * (2 * STEP)
    out = jax.eval_shape(first_state, moments, Pair(s, s), s)
    return jax.tree_util.tree_flatten(out)


def summed_moments(gathered):
    rows = gathered.shape[0] // 8
    zero = jnp.zeros((8, LANES), F32)
    terms = [Pair(gathered[8 * i : 8 * i + 8], zero) for i in range(rows)]
    while len(terms) > 1:
        terms = [terms[i] + terms[i + 1] for i in range(0, len(terms) - 1, 2)] + (
            [terms[-1]] if len(terms) % 2 else []
        )
    t = terms[0]
    for s in (4, 2, 1):
        t = t + Pair(pltpu.roll(t.h, s, 0), pltpu.roll(t.l, s, 0))
    width = LANES // (2 * STEP)
    s = width // 2
    while s:
        t = t + Pair(pltpu.roll(t.h, LANES - s, 1), pltpu.roll(t.l, LANES - s, 1))
        s //= 2
    lane = lax.broadcasted_iota(jnp.int32, (8, LANES), 1)

    def spread(v, j):
        picked = jnp.where(lane == width * j, v, 0.0)
        return jnp.broadcast_to(jnp.sum(picked, axis=1, keepdims=True), (8, LANES))

    return [Pair(spread(t.h, j), spread(t.l, j)) for j in range(2 * STEP)]


def vm(n):
    return [pl.BlockSpec(memory_space=pltpu.VMEM)] * n


def call(body, name, outs, args, smem=0, scratch=()):
    specs = [pl.BlockSpec(memory_space=pltpu.SMEM)] * smem + vm(len(args) - smem)
    return pl.pallas_call(
        body,
        name=name,
        in_specs=specs,
        out_specs=vm(len(outs)),
        out_shape=[jax.ShapeDtypeStruct(s, F32) for s in outs],
        scratch_shapes=list(scratch),
        compiler_params=pltpu.CompilerParams(vmem_limit_bytes=24 * 1024 * 1024),
    )(*args)


def fold_kernel(where, own, other, source, out):
    first = where[0] == 0
    edge = jnp.where(where[1] == 1, -1.0, 1.0).astype(F32)
    xs, ts = source.shape[3], source.shape[4]
    shape = (ts, LANES)
    lane = lax.broadcasted_iota(jnp.int32, shape, 1)
    row = lax.broadcasted_iota(jnp.int32, shape, 0)
    y = lane // NZ
    yz = y + lane % NZ
    for x in range(xs):
        signs = [
            jnp.full(shape, 0.5, F32),
            jnp.full(shape, 0.5 if x % 2 == 0 else -0.5, F32),
            jnp.where((y + x) % 2 == 0, 0.5, -0.5).astype(F32),
            jnp.where((yz + x) % 2 == 0, 0.5, -0.5).astype(F32)
            * jnp.where(row == ts - 1, edge, 1.0),
        ]
        for mu in range(4):
            for k in range(18):
                p, r, c = k // 9, (k // 3) % 3, k % 3
                a = own[mu % 2, p, r, c, x]
                b = other[mu % 2, p, r, c, x]
                w = jnp.where(first, a, b) if mu < 2 else jnp.where(first, b, a)
                out[18 * mu + k, x] = w * signs[mu]
        for k in range(6):
            out[72 + k, x] = source[0, k // 3, k % 3, x]


def widen(out, index, low, own, high):
    ts = own.shape[0]
    out[(*index, slice(0, ts))] = low
    out[(*index, slice(ts, 2 * ts))] = own
    out[(*index, slice(2 * ts, 3 * ts))] = high
    out[(*index, slice(3 * ts, ROWS))] = jnp.zeros((ROWS - 3 * ts, LANES), F32)


def wide_links_kernel(own, low, high, out, up, down):
    n = own.shape[0]

    def one(k, _):
        for x in range(2):
            widen(out, (k, x), low[k, x], own[k, x], high[k, x])
        return 0

    lax.fori_loop(0, n, one, 0)

    def copy(k, _):
        up[k] = out[k, 1]
        down[k] = out[k, 0]
        return 0

    lax.fori_loop(0, 72, copy, 0)
    for k in range(18):
        up[72 + k] = out[k, 0]
    for k in range(6):
        for x in range(2):
            up[90 + 2 * k + x] = out[72 + k, x]
            down[72 + 2 * k + x] = out[72 + k, x]


def wide_field_kernel(own, low, high, out):
    for k in range(6):
        for x in range(2):
            widen(out, (k, x), low[k, x], own[k, x], high[k, x])


def lanes_of(shape):
    return lax.broadcasted_iota(jnp.int32, shape, 1) % NZ


def z_ahead(v, vy, z):
    return jnp.where(z == NZ - 1, pltpu.roll(vy, LANES - 1, 1), pltpu.roll(v, LANES - 1, 1))


def z_behind(v, vy, z):
    return jnp.where(z == 0, pltpu.roll(vy, 1, 1), pltpu.roll(v, 1, 1))


def times(acc, link, v):
    for r in range(3):
        for c in range(3):
            re, im = link(3 * r + c), link(9 + 3 * r + c)
            acc[r] = acc[r] + re * v[c] - im * v[3 + c]
            acc[3 + r] = acc[3 + r] + re * v[3 + c] + im * v[c]


def less_adjoint(acc, link, v):
    for r in range(3):
        for c in range(3):
            re, im = link(3 * c + r), link(9 + 3 * c + r)
            acc[r] = acc[r] - re * v[c] - im * v[3 + c]
            acc[3 + r] = acc[3 + r] - re * v[3 + c] + im * v[c]


def hop(src, dst, rows, base, links):
    lx, ly, lz, lzb, lt, ltb = links
    z = lanes_of((ROWS, LANES))

    def one(i, _):
        acc = [jnp.zeros((ROWS, LANES), F32)] * 6
        s = base + i
        times(acc, lambda k: lx[k, s + 1], [src[k, i + 2] for k in range(6)])
        less_adjoint(acc, lambda k: lx[k, s], [src[k, i] for k in range(6)])
        v = [src[k, i + 1] for k in range(6)]
        times(acc, lambda k: lt[k, s], [pltpu.roll(u, ROWS - 1, 0) for u in v])
        less_adjoint(acc, lambda k: ltb[k, s], [pltpu.roll(u, 1, 0) for u in v])
        vy = [pltpu.roll(u, NZ, 1) for u in v]
        times(acc, lambda k: ly[k, s], vy)
        times(acc, lambda k: lz[k, s], [z_ahead(u, w, z) for u, w in zip(v, vy)])
        less_adjoint(acc, lambda k: lzb[k, s], [z_behind(u, w, z) for u, w in zip(v, vy)])
        for k in range(6):
            dst[k, i] = acc[k]
        return 0

    lax.fori_loop(0, rows, one, 0)


def norm_row(src, x0, moments, j):
    row = lax.broadcasted_iota(jnp.int32, (8, LANES), 0)
    t = jnp.zeros((8, LANES), F32)
    for k in range(6):
        for x in range(2):
            v = src[k, x0 + x, 0:8]
            t = t + v * v
    t = jnp.sum(jnp.where(row >= 4, t, 0.0), axis=0, keepdims=True)
    return jnp.where(row == j, jnp.broadcast_to(t, (8, LANES)), moments)


def build_links(own, low, high, links):
    lx, ly, lz, lzb, lt, ltb = links
    z = lanes_of((ROWS, LANES))
    for k in range(18):
        lx[k, 0] = low[72 + k]
        lx[k, 1] = low[k]
        lx[k, 2] = own[k, 0]
        lx[k, 3] = own[k, 1]
        lx[k, 4] = high[k]

    for i in range(4):

        def at(k, i=i):
            return low[k] if i == 0 else high[k] if i == 3 else own[k, i - 1]

        for r in range(3):
            for c in range(3):
                k, a = 3 * r + c, 3 * c + r
                ly[k, i] = at(18 + k) - pltpu.roll(at(18 + a), NZ, 1)
                ly[9 + k, i] = at(27 + k) + pltpu.roll(at(27 + a), NZ, 1)
        for k in range(18):
            w = at(36 + k)
            lz[k, i] = w
            lzb[k, i] = z_behind(w, pltpu.roll(w, NZ, 1), z)
            w = at(54 + k)
            lt[k, i] = w
            ltb[k, i] = pltpu.roll(w, 1, 0)


def first_hops_kernel(own, low, high, out, moments, lx, ly, lz, lzb, lt, ltb, v0, v1):
    links = (lx, ly, lz, lzb, lt, ltb)
    build_links(own, low, high, links)
    for k in range(6):
        for x in range(2):
            v0[k, x] = low[90 + 2 * k + x]
            v0[k, 2 + x] = own[72 + k, x]
            v0[k, 4 + x] = high[72 + 2 * k + x]
    hop(v0, v1, 4, 0, links)
    hop(v1, out, 2, 1, links)
    m = norm_row(v0, 2, jnp.zeros((8, LANES), F32), 0)
    m = norm_row(v1, 1, m, 1)
    moments[...] = norm_row(out, 0, m, 2)


def message_row(m):
    s = LANES // 2
    while s >= LANES // (2 * STEP):
        m = m + pltpu.roll(m, s, 1)
        s //= 2
    row = lax.broadcasted_iota(jnp.int32, (8, LANES), 0)
    lane = lax.broadcasted_iota(jnp.int32, (8, LANES), 1)
    m = jnp.where(lane // (LANES // (2 * STEP)) == row, m, 0.0)
    return jnp.sum(m, axis=0, keepdims=True)


def hops_kernel(j, local, send, hops, own, low, high, before, lx, ly, lz, lzb, lt, ltb, *rest):
    links = (lx, ly, lz, lzb, lt, ltb)
    out, moments, v0, v1, v2 = rest
    for k in range(6):
        for x in range(2):
            v0[k, x] = low[k, x]
            v0[k, 2 + x] = own[k, x]
            v0[k, 4 + x] = high[k, x]
    m = before[...] if before is not None else None
    if j == 1:
        m = norm_row(v0, 2, jnp.zeros((8, LANES), F32), 0)
    if hops == 1:
        hop(v0.at[:, 1:5], v2, 2, 1, links)
        m = norm_row(v2, 0, m, j)
    else:
        dst = v2 if local else out
        hop(v0, v1, 4, 0, links)
        hop(v1, dst, 2, 1, links)
        m = norm_row(v1, 1, m, j)
        if j + 1 < 2 * STEP:
            m = norm_row(dst, 0, m, j + 1)
    if local:
        for k in range(6):
            for x in range(2):
                out[k, x] = v2[k, x, 4:8]
    moments[...] = message_row(m) if send else m


def field_rows(ref, k, x):
    if ref.ndim == 6:
        return ref[0, k // 3, k % 3, x]
    v = ref[k, x]
    return v if v.shape[0] == 4 else v[4:8]


def restart_kernel(mass, gathered, shifts, b, hb, h2b, h3b, h4b, out, state):
    one = jnp.ones((8, LANES), F32)
    m = jnp.full((8, LANES), mass[0], F32)
    m2 = Pair(m * m, jnp.zeros_like(one))
    s = first_state(summed_moments(gathered[...]), m2, shifts[...])
    leaves, _ = jax.tree_util.tree_flatten(s)
    for i, leaf in enumerate(leaves):
        state[i : i + 1] = leaf[0:1]
    rest, top = s["handover"]
    c = [rest[0], -rest[1], rest[2], -rest[3], top]
    c = [v[0:4] for v in c]
    for k in range(6):
        for x in range(2):
            t = c[0] * field_rows(b, k, x)
            for w, ref in zip(c[1:], (hb, h2b, h3b, h4b)):
                t = t + w * field_rows(ref, k, x)
            out[k, x] = t


def finish_kernel(tree, mass, gathered, shifts, residues, state, before, *refs):
    fields, out, act = refs[:8], refs[8], refs[9]
    one = jnp.ones((8, LANES), F32)
    m = jnp.full((8, LANES), mass[0], F32)
    m2 = Pair(m * m, jnp.zeros_like(one))
    leaves = [
        jnp.broadcast_to(state[i : i + 1], (8, LANES)) for i in range(tree.num_leaves)
    ]
    s = jax.tree_util.tree_unflatten(tree, leaves)
    s = run_steps(STEP, summed_moments(gathered[...]), s, m2, one, shifts[...], True)
    weights = residues[...]
    c = [
        jnp.broadcast_to(
            jnp.sum(weights * s["sol"][j], axis=1, keepdims=True), (8, LANES)
        )
        for j in range(2 * STEP)
    ]
    powers = summed_moments(before[...])
    t = c[0] * powers[0].h
    for j in range(1, STEP):
        t = t + c[j] * powers[j].h
    act[...] = t
    c = [(v if j % 2 == 0 else -v)[0:4] for j, v in enumerate(c)]
    for k in range(6):
        for x in range(2):
            t = c[0] * field_rows(fields[0], k, x)
            for w, ref in zip(c[1:], fields[1:]):
                t = t + w * field_rows(ref, k, x)
            out[0, k // 3, k % 3, x] = t


def both_ways(x_up, x_down, axis):
    n = lax.axis_size(axis)
    up = [(i, (i + 1) % n) for i in range(n)]
    return lax.ppermute(x_up, axis, up), lax.ppermute(x_down, axis, [(b, a) for a, b in up])


def everyone(row):
    n = lax.axis_size(ZT_XY)
    rows = lax.all_to_all(jnp.broadcast_to(row[None], (n, 1, LANES)), ZT_XY, 0, 0, tiled=True)
    rows = rows.reshape(n, LANES)
    return jnp.pad(rows, ((0, -n % 8), (0, 0)))


def field_scratch():
    return [pltpu.VMEM((6, n, ROWS, LANES), F32) for n in (6, 4, 2)]


def on_device(source, links, shifts, residues, mass):
    grp = lax.axis_index("grp")
    xs, ts = source.shape[3], source.shape[4]
    last = lax.axis_index(ZT) == lax.axis_size(ZT) - 1
    where = jnp.stack([grp, last.astype(jnp.int32)])
    lane_shifts = jnp.broadcast_to(
        jnp.pad(shifts, (0, LANES - shifts.shape[0]), constant_values=1.0), (8, LANES)
    )
    lane_residues = jnp.broadcast_to(
        jnp.pad(residues, (0, LANES - residues.shape[0])), (8, LANES)
    )
    other = lax.ppermute(links, "grp", [(0, 1), (1, 0)])
    small = (6, xs, ts, LANES)
    tall = (6, xs, ROWS, LANES)
    (mine,) = call(fold_kernel, "fold", [(78, xs, ts, LANES)], (where, links, other, source), 1)
    low, high = both_ways(mine, mine, ZT)
    wide, up, down = call(
        wide_links_kernel,
        "wide_links",
        [(78, xs, ROWS, LANES), (102, ROWS, LANES), (84, ROWS, LANES)],
        (mine, low, high),
    )
    low, high = both_ways(up, down, XY)
    shapes = [(18, LX_N, ROWS, LANES)] + [(18, L_N, ROWS, LANES)] * 5
    f2, m, *w = call(
        first_hops_kernel,
        "first_hops",
        [tall, (8, LANES), *shapes],
        (wide, low, high),
        scratch=field_scratch()[:2],
    )

    def hops(field, m, j, local, send=False, count=2):
        low, high = both_ways(field, field, XY)
        first = m is None
        body = functools.partial(hops_kernel, j, local, send, count)
        if first:
            plain = body

            def body(own, low, high, *rest):
                plain(own, low, high, None, *rest)

        args = (field, low, high) + (() if first else (m,)) + tuple(w)
        out, m = call(
            body,
            "hops",
            [small if local else tall, (1, LANES) if send else (8, LANES)],
            args,
            scratch=field_scratch(),
        )
        return out, m

    def taller(field):
        low, high = both_ways(field, field, ZT)
        return call(wide_field_kernel, "wide_field", [tall], (field, low, high))[0]

    f4, m = hops(f2, m, 3, True)
    f6, m = hops(taller(f4), m, 5, False)
    f8, m = hops(f6, m, 7, True, True)
    gathered = everyone(m)
    leaves, tree = state_shape()
    count = -(-len(leaves) // 8) * 8
    r0, state = call(
        restart_kernel,
        "restart",
        [small, (count, LANES)],
        (mass, gathered, lane_shifts, source, f2, f4, f6, f8),
        1,
    )
    r2, m = hops(taller(r0), None, 1, False)
    r4, m = hops(r2, m, 3, True)
    r6, m = hops(taller(r4), m, 5, False)
    _, m = hops(r6, m, 7, True, True, 1)
    rational, act = call(
        functools.partial(finish_kernel, tree),
        "finish",
        [source.shape, (8, LANES)],
        (mass, everyone(m), lane_shifts, lane_residues, state, gathered)
        + (source, f2, f4, f6, r0, r2, r4, r6),
        1,
    )
    act = act[0:1]
    total = act + lax.ppermute(act, "grp", [(0, 1), (1, 0)])
    sites = xs * lax.axis_size(XY) * ts * lax.axis_size(ZT) * LANES
    sites *= source.shape[0] * lax.axis_size("grp")
    return (rational, (total / sites)[0, 0:1])


def solution(mesh):
    if mesh.size == 512:
        shape = (mesh.shape["grp"], 4, 4, 8, 2)
    else:
        shape = (mesh.shape["grp"], mesh.shape["zt"], 1, mesh.shape["xy"], 1)
    torus = Mesh(mesh.devices.reshape(shape), ("grp", "zt_0", "zt_1", "xy_0", "xy_1"))
    placed = (
        P("grp", None, None, XY, ZT, None),
        P("grp", None, None, None, XY, ZT, None),
        P(),
        P(),
        P(),
    )
    return jax.shard_map(
        on_device,
        mesh=torus,
        in_specs=placed,
        out_specs=(P("grp", None, None, XY, ZT, None), P()),
        check_vma=False,
    )
```

```python
import functools

import jax
import jax.numpy as jnp
from jax import lax
from jax.experimental import pallas as pl
from jax.experimental.pallas import tpu as pltpu
from jax.sharding import Mesh
from jax.sharding import PartitionSpec as P

NY = 2
NZ = 64
LANES = NY * NZ
STEP = 4
XY = ("xy_0", "xy_1")
ZT = ("zt_0", "zt_1")
ZT_XY = ("zt_0", "zt_1", "xy_0", "xy_1")
F32 = jnp.float32
ROWS = 16
REDUCE = ("zt_0", "zt_1", "xy_0")
LOCAL = (6, 8, LANES)


def two_sum(a, b):
    s = a + b
    t = s - a
    return s, (a - (s - t)) + (b - t)


def quick_sum(a, b):
    s = a + b
    return s, b - (s - a)


def halves(a):
    t = a * 4097.0
    h = t - (t - a)
    return h, a - h


def two_prod(a, b):
    p = a * b
    ah, al = halves(a)
    bh, bl = halves(b)
    return p, ((ah * bh - p) + ah * bl + al * bh) + al * bl


@jax.tree_util.register_pytree_node_class
class Pair:
    def __init__(self, h, l):
        self.h = h
        self.l = l

    def tree_flatten(self):
        return (self.h, self.l), None

    @classmethod
    def tree_unflatten(cls, _, leaves):
        return cls(*leaves)

    def __add__(self, o):
        a, e = two_sum(self.h, o.h)
        t, f = two_sum(self.l, o.l)
        a, e = quick_sum(a, e + t)
        return Pair(*quick_sum(a, e + f))

    def __neg__(self):
        return Pair(-self.h, -self.l)

    def __sub__(self, o):
        return self + (-o)

    def __mul__(self, o):
        p, e = two_prod(self.h, o.h)
        return Pair(*quick_sum(p, e + (self.h * o.l + self.l * o.h)))

    def times(self, f):
        p, e = two_prod(self.h, f)
        return Pair(*quick_sum(p, e + self.l * f))

    def __truediv__(self, o):
        q1 = self.h / o.h
        r = self - o.times(q1)
        q2 = r.h / o.h
        r = r - o.times(q2)
        a, b = quick_sum(q1, q2)
        return Pair(*quick_sum(a, b + r.h / o.h))


def plus(a, b):
    return b if a is None else a + b


def run_steps(first, moments, state, m2, one, shifts, final):
    size = STEP
    al, be, c, gam = (dict(state[n]) for n in ("al", "be", "c", "gam"))
    coef = dict(state["coef"])
    part, sol = dict(state["part"]), dict(state["sol"])
    zeta, zeta_old, zeta_new = state["zeta"], state["zeta_old"], state["zeta_new"]
    unit = Pair(one, jnp.zeros_like(one))
    table = {first: list(moments)}
    raised = {}
    if first:
        inv, own, low = {}, {}, {}
        for k in range(first):
            inv[k] = unit / al[k]
            own[k] = (unit + c[k] if k else unit) * inv[k] - m2
            if k:
                low[k] = c[k] * inv[k]
            table[k] = [None] * (2 * size)
        for i in range(1, 2 * size):
            for k in range(first - 1, -1, -1):
                if i < first - k:
                    continue
                t = None
                if table[k][i - 1] is not None:
                    t = plus(t, own[k] * table[k][i - 1])
                if table[k + 1][i - 1] is not None:
                    t = plus(t, -(inv[k] * table[k + 1][i - 1]))
                if k and table[k - 1][i - 1] is not None:
                    t = plus(t, -(low[k] * table[k - 1][i - 1]))
                table[k][i] = t
        rest, top = state["handover"]
        scale = one / top
        for k in range(first - 1):
            raised[k] = {k + 1: one}
        raised[first - 1] = {j: -(rest[j] * scale) for j in rest}
        raised[first - 1][first] = scale
    for i in range(size - 1):
        raised[first + i] = {first + i + 1: one}
    coef[first] = {first: one}
    lead, second = unit, None
    handover = None
    for d in range(size):
        k = first + d
        norm = lead * table[k][d]
        high = lead * table[k][d + 1]
        if second is not None:
            high = high + second * table[k][d]
        gam[k] = norm
        if k == 0:
            part = {0: jnp.ones_like(shifts)}
        else:
            ratio = norm / gam[k - 1]
            be[k - 1] = ratio
            step = zeta_new / zeta
            keep = ratio.h * step * step
            grown = {}
            for j in sorted(set(part) | set(coef[k])):
                t = None
                if j in coef[k]:
                    t = zeta_new * coef[k][j]
                if j in part:
                    t = plus(t, keep * part[j])
                grown[j] = t
            part = grown
            zeta_old, zeta = zeta, zeta_new
        curve = m2 * norm + high
        if k:
            curve = curve - ratio * norm / al[k - 1]
        a = norm / curve
        al[k] = a
        if k:
            a_old, b_old = al[k - 1].h, be[k - 1].h
            zeta_new = (
                zeta
                * zeta_old
                * a_old
                / (a.h * b_old * (zeta_old - zeta) + zeta_old * a_old * (1.0 + shifts * a.h))
            )
            c[k] = a * be[k - 1] / al[k - 1]
            keep_r = unit + c[k]
        else:
            zeta_new = zeta / (1.0 + shifts * a.h)
            keep_r = unit
        gain = a.h * zeta_new / zeta
        for j in part:
            sol[j] = plus(sol.get(j), gain * part[j])
        if d == size - 1 and final:
            break
        image = {}
        for j, v in coef[k].items():
            image[j] = plus(image.get(j), m2.h * v)
            if j == first + size - 1:
                continue
            for jj, w in raised[j].items():
                image[jj] = plus(image.get(jj), w * v)
        following = {}
        for j in sorted(set(coef[k]) | set(image) | set(coef.get(k - 1, {}))):
            t = None
            if j in coef[k]:
                t = keep_r.h * coef[k][j]
            if j in image:
                t = plus(t, -(a.h * image[j]))
            if k and j in coef[k - 1]:
                t = plus(t, -(c[k].h * coef[k - 1][j]))
            following[j] = t
        if d == size - 1:
            handover = (following, -(a.h * coef[k][first + size - 1]))
            break
        coef[k + 1] = following
        row = [None] * (2 * size)
        for i in range(2 * size - 1 - d):
            if table[k][i] is None or table[k][i + 1] is None:
                continue
            t = keep_r * table[k][i] - a * (m2 * table[k][i] + table[k][i + 1])
            if k and table[k - 1][i] is not None:
                t = t - c[k] * table[k - 1][i]
            row[i] = t
        table[k + 1] = row
        image_second = m2 * lead if second is None else m2 * lead + second
        lead, second = -(a * lead), keep_r * lead - a * image_second
    last = first + size - 1
    return {
        "al": al,
        "be": be,
        "c": c,
        "gam": {last: gam[last]},
        "coef": {last: coef[last]},
        "part": part,
        "sol": sol,
        "zeta": zeta,
        "zeta_old": zeta_old,
        "zeta_new": zeta_new,
        "handover": handover,
    }


def start_state(one):
    return {
        "al": {},
        "be": {},
        "c": {},
        "gam": {},
        "coef": {},
        "part": {},
        "sol": {},
        "zeta": one,
        "zeta_old": one,
        "zeta_new": one,
        "handover": None,
    }


def first_state(moments, m2, shifts):
    one = jnp.ones_like(shifts)
    return run_steps(0, moments, start_state(one), m2, one, shifts, False)


def summed_moments(gathered):
    rows = gathered.shape[0] // 8
    zero = jnp.zeros((8, LANES), F32)
    terms = [Pair(gathered[8 * i : 8 * i + 8], zero) for i in range(rows)]
    while len(terms) > 1:
        terms = [terms[i] + terms[i + 1] for i in range(0, len(terms) - 1, 2)] + (
            [terms[-1]] if len(terms) % 2 else []
        )
    t = terms[0]
    for s in (4, 2, 1):
        t = t + Pair(pltpu.roll(t.h, s, 0), pltpu.roll(t.l, s, 0))
    width = LANES // (2 * STEP)
    s = width // 2
    while s:
        t = t + Pair(pltpu.roll(t.h, LANES - s, 1), pltpu.roll(t.l, LANES - s, 1))
        s //= 2
    lane = lax.broadcasted_iota(jnp.int32, (8, LANES), 1)

    def spread(v, j):
        picked = jnp.where(lane == width * j, v, 0.0)
        return jnp.broadcast_to(jnp.sum(picked, axis=1, keepdims=True), (8, LANES))

    return [Pair(spread(t.h, j), spread(t.l, j)) for j in range(2 * STEP)]


def call(body, name, outs, args, smem=0, far=0, scratch=()):
    n = len(args)
    specs = [pl.BlockSpec(memory_space=pltpu.SMEM)] * smem
    specs += [pl.BlockSpec(memory_space=pltpu.VMEM)] * (n - smem - far)
    specs += [pl.BlockSpec(memory_space=pl.ANY)] * far
    return pl.pallas_call(
        body,
        name=name,
        in_specs=specs,
        out_specs=[pl.BlockSpec(memory_space=pltpu.VMEM)] * len(outs),
        out_shape=[jax.ShapeDtypeStruct(s, F32) for s in outs],
        scratch_shapes=list(scratch),
        compiler_params=pltpu.CompilerParams(vmem_limit_bytes=12 * 1024 * 1024),
    )(*args)


def wide_links_kernel(where, own, low, high, own_x, low_x, high_x, out, up, down):
    first = where[0] == 0
    flip = [jnp.where(where[i] == 1, -1.0, 1.0).astype(F32) for i in (1, 2, 3)]
    shape = (8, LANES)
    lane = lax.broadcasted_iota(jnp.int32, shape, 1)
    row = lax.broadcasted_iota(jnp.int32, shape, 0)
    x, t = row // 4, row % 4
    y = lane // NZ
    z = lane % NZ
    half = jnp.full(shape, 0.5, F32)
    etas = [
        half,
        jnp.where(x % 2 == 0, half, -half),
        jnp.where((x + y) % 2 == 0, half, -half),
        jnp.where((x + y + z) % 2 == 0, half, -half),
    ]
    zero = jnp.zeros((4, LANES), F32)
    sides = ((low, low_x), (own, own_x), (high, high_x))

    def place(k, parts):
        for i in range(2):
            cut = [v[4 * i : 4 * i + 4] for v in parts]
            out[k, i, 0:4] = cut[0]
            out[k, i, 4:8] = cut[1]
            out[k, i, 8:12] = cut[2]
            out[k, i, 12:16] = zero

    for mu in range(4):
        signs = [
            jnp.where(t == 3, etas[mu] * flip[i], etas[mu]) if mu == 3 else etas[mu]
            for i in range(3)
        ]

        def one(k, _, mu=mu, signs=signs):
            j = 18 * (mu % 2) + k
            parts = []
            for (a, b), s in zip(sides, signs):
                mine, theirs = a[j], b[j]
                w = jnp.where(first, mine, theirs) if mu < 2 else jnp.where(first, theirs, mine)
                parts.append(w * s)
            place(18 * mu + k, parts)
            return 0

        lax.fori_loop(0, 18, one, 0)
    for k in range(6):
        place(72 + k, [a[36 + k] for a, _ in sides])

    def pack(k, _):
        for i in range(2):
            up[2 * k + i] = out[2 * k + i, 1, 0:8]
            down[2 * k + i] = out[2 * k + i, 0, 0:8]
            up[102 + k, 4 * i : 4 * i + 4] = out[2 * k + i, 1, 8:12]
            down[84 + k, 4 * i : 4 * i + 4] = out[2 * k + i, 0, 8:12]
        return 0

    lax.fori_loop(0, 36, pack, 0)
    for k in range(9):
        for i in range(2):
            up[72 + 2 * k + i] = out[2 * k + i, 0, 0:8]
            up[138 + k, 4 * i : 4 * i + 4] = out[2 * k + i, 0, 8:12]
    for k in range(6):
        for i in range(2):
            up[90 + 2 * k + i] = out[72 + k, i, 0:8]
            down[72 + 2 * k + i] = out[72 + k, i, 0:8]
            up[147 + k, 4 * i : 4 * i + 4] = out[72 + k, i, 8:12]
            down[120 + k, 4 * i : 4 * i + 4] = out[72 + k, i, 8:12]


UP_N = 153
DOWN_N = 126


def wide_field_kernel(own, low, high, out):
    for k in range(6):
        for x in range(2):
            c = slice(4 * x, 4 * x + 4)
            out[2 * k + x, 0:4] = low[k, c]
            out[2 * k + x, 4:8] = own[k, c]
            out[12 + k, c] = high[k, c]


def put_wide(dst, k, x, msg):
    dst[0:8] = msg[2 * k + x]
    dst[8:12] = msg[12 + k, 4 * x : 4 * x + 4]


def z_ahead(v, vy, z):
    return jnp.where(z == NZ - 1, pltpu.roll(vy, LANES - 1, 1), pltpu.roll(v, LANES - 1, 1))


def z_behind(v, vy, z):
    return jnp.where(z == 0, pltpu.roll(vy, 1, 1), pltpu.roll(v, 1, 1))


def times(acc, link, v):
    for r in range(3):
        for c in range(3):
            re, im = link(3 * r + c), link(9 + 3 * r + c)
            acc[r] = acc[r] + re * v[c] - im * v[3 + c]
            acc[3 + r] = acc[3 + r] + re * v[3 + c] + im * v[c]


def adjoint(link, v):
    acc = [None] * 6
    for r in range(3):
        for c in range(3):
            re, im = link(3 * c + r), link(9 + 3 * c + r)
            acc[r] = plus(acc[r], re * v[c] + im * v[3 + c])
            acc[3 + r] = plus(acc[3 + r], re * v[3 + c] - im * v[c])
    return acc


def hop(src, dst, rows, base, links):
    lx, ly, lz, lt = links
    z = lax.broadcasted_iota(jnp.int32, (ROWS, LANES), 1) % NZ

    def one(i, _):
        s = base + i
        v = [src[k, i + 1] for k in range(6)]
        vy = [pltpu.roll(u, NZ, 1) for u in v]
        back = adjoint(lambda k: lz[k, s], v)
        acc = [-z_behind(u, pltpu.roll(u, NZ, 1), z) for u in back]
        times(acc, lambda k: lz[k, s], [z_ahead(u, w, z) for u, w in zip(v, vy)])
        times(acc, lambda k: ly[k, s], vy)
        back = adjoint(lambda k: lt[k, s], v)
        acc = [a - pltpu.roll(u, 1, 0) for a, u in zip(acc, back)]
        times(acc, lambda k: lt[k, s], [pltpu.roll(u, ROWS - 1, 0) for u in v])
        times(acc, lambda k: lx[k, s + 1], [src[k, i + 2] for k in range(6)])
        back = adjoint(lambda k: lx[k, s], [src[k, i] for k in range(6)])
        for k in range(6):
            dst[k, i] = acc[k] - back[k]
        return 0

    lax.fori_loop(0, rows, one, 0)


def put_local(out, src, x0):
    t = None
    for k in range(6):
        for x in range(2):
            out[k, 4 * x : 4 * x + 4] = src[k, x0 + x, 4:8]
        t = plus(t, out[k] * out[k])
    return jnp.sum(t, axis=0, keepdims=True)


def set_row(moments, j, t):
    row = lax.broadcasted_iota(jnp.int32, (8, LANES), 0)
    return jnp.where(row == j, jnp.broadcast_to(t, (8, LANES)), moments)


def message_row(m):
    s = LANES // 2
    while s >= LANES // (2 * STEP):
        m = m + pltpu.roll(m, s, 1)
        s //= 2
    row = lax.broadcasted_iota(jnp.int32, (8, LANES), 0)
    lane = lax.broadcasted_iota(jnp.int32, (8, LANES), 1)
    m = jnp.where(lane // (LANES // (2 * STEP)) == row, m, 0.0)
    return jnp.sum(m, axis=0, keepdims=True)


def two_hops(j, send, m, v0, v1, v2, links, odd, even, ahead, moments):
    hop(v0, v1, 4, 0, links)
    hop(v1, v2, 2, 1, links)
    t = put_local(odd, v1, 1)
    m = set_row(m, j, t) if j < 2 * STEP else m
    t = put_local(even, v2, 0)
    m = set_row(m, j + 1, t) if j + 1 < 2 * STEP else m
    if ahead is not None:
        for k in range(6):
            for x in range(2):
                ahead[2 * k + x] = v2[k, x, 2:10]
    moments[...] = message_row(m) if send else m


def first_hops_kernel(own, low, high, ahead, odd, even, moments, lx, ly, lz, lt, v0, v1, v2):
    links = (lx, ly, lz, lt)

    def side(msg, i, half):
        def at(k):
            c = 4 * (k % 2)
            return msg[i + k], msg[half + k // 2, slice(c, c + 4)]

        return at

    def store(dst, pieces):
        dst[0:8] = pieces[0]
        dst[8:12] = pieces[1]
        dst[12:16] = jnp.zeros((4, LANES), F32)

    behind, behind2, ahead1 = side(low, 0, 102), side(low, 72, 138), side(high, 0, 84)
    for k in range(18):
        store(lx.at[k, 0], behind2(k))
        store(lx.at[k, 1], behind(k))
        lx[k, 2] = own[k, 0]
        lx[k, 3] = own[k, 1]
        store(lx.at[k, 4], ahead1(k))
        for i, ref in ((36, lz), (54, lt)):
            store(ref.at[k, 0], behind(i + k))
            ref[k, 1] = own[i + k, 0]
            ref[k, 2] = own[i + k, 1]
            store(ref.at[k, 3], ahead1(i + k))
        store(v2.at[0, 0], behind(18 + k))
        store(v2.at[0, 1], ahead1(18 + k))
        c, r = (k % 9) % 3, (k % 9) // 3
        ly[k, 0] = v2[0, 0]
        ly[k, 1] = own[18 + k, 0]
        ly[k, 2] = own[18 + k, 1]
        ly[k, 3] = v2[0, 1]
    for i in range(4):
        for r in range(3):
            for c in range(r + 1):
                k, a = 3 * r + c, 3 * c + r
                u, w = ly[k, i], ly[a, i]
                ur, wr = pltpu.roll(u, NZ, 1), pltpu.roll(w, NZ, 1)
                ly[k, i] = u - wr
                if a != k:
                    ly[a, i] = w - ur
                u, w = ly[9 + k, i], ly[9 + a, i]
                ur, wr = pltpu.roll(u, NZ, 1), pltpu.roll(w, NZ, 1)
                ly[9 + k, i] = u + wr
                if a != k:
                    ly[9 + a, i] = w + ur
    m = jnp.zeros((8, LANES), F32)
    t = None
    for k in range(6):
        for x in range(2):
            c = slice(4 * x, 4 * x + 4)
            v0[k, x, 0:8] = low[90 + 2 * k + x]
            v0[k, x, 8:12] = low[147 + k, c]
            v0[k, 2 + x] = own[72 + k, x]
            v0[k, 4 + x, 0:8] = high[72 + 2 * k + x]
            v0[k, 4 + x, 8:12] = high[120 + k, c]
            v = own[72 + k, x, 4:8]
            t = plus(t, v * v)
    m = set_row(m, 0, jnp.sum(t, axis=0, keepdims=True))
    two_hops(1, False, m, v0, v1, v2, links, odd, even, ahead, moments)


def hops_kernel(j, kind, own, low, high, before, lx, ly, lz, lt, *rest):
    links = (lx, ly, lz, lt)
    outs, (v0, v1, v2) = rest[:-3], rest[-3:]
    for k in range(6):
        for x in range(2):
            for i, ref in ((0, low), (2, own), (4, high)):
                if kind == "wide":
                    put_wide(v0.at[k, i + x], k, x, ref)
                else:
                    v0[k, i + x, 2:10] = ref[2 * k + x]
    m = before[...]
    if kind == "wide":
        ahead, odd, even, moments = outs
        two_hops(j, False, m, v0, v1, v2, links, odd, even, ahead, moments)
    elif kind == "next":
        odd, even, moments = outs
        two_hops(j, j + 1 == 2 * STEP, m, v0, v1, v2, links, odd, even, None, moments)
    else:
        (moments,) = outs
        hop(v0.at[:, 1:5], v2, 2, 1, links)
        t = None
        for k in range(6):
            for x in range(2):
                v = v2[k, x, 4:8]
                t = plus(t, v * v)
        m = set_row(m, j, jnp.sum(t, axis=0, keepdims=True))
        moments[...] = message_row(m)


def start_copies(fields, held, sems):
    copies = [pltpu.make_async_copy(f, held.at[i], sems.at[i]) for i, f in enumerate(fields)]
    for c in copies:
        c.start()
    return copies


def restart_kernel(mass, gathered, shifts, *refs):
    n = 3 * STEP + 1
    fields, (r0, r2, r4, moments, state, held, sems) = refs[:n], refs[n:]
    copies = start_copies(fields, held, sems)
    one = jnp.ones((8, LANES), F32)
    m = jnp.full((8, LANES), mass[0], F32)
    m2 = Pair(m * m, jnp.zeros_like(one))
    powers = summed_moments(gathered[...])
    s = first_state(powers, m2, shifts[...])
    leaves, _ = jax.tree_util.tree_flatten((s, [p.h for p in powers[:STEP]]))
    for i, leaf in enumerate(leaves):
        state[i : i + 1] = leaf[0:1]
    rest, top = s["handover"]
    c = [rest[0], -rest[1], rest[2], -rest[3], top]
    for copy in copies:
        copy.wait()
    row = jnp.zeros((8, LANES), F32)
    for i in range(STEP + 1):
        out = {0: r0, 2: r2, 4: r4}.get(i)
        square = None
        for k in range(6):
            t = None
            for j in range(STEP + 1):
                t = plus(t, c[j] * held[i + 2 * j, k])
            if out is not None:
                out[k] = t
            square = plus(square, t * t)
        row = set_row(row, i, jnp.sum(square, axis=0, keepdims=True))
    moments[...] = row


def finish_kernel(tree, mass, gathered, shifts, residues, state, *refs):
    n = 2 * STEP
    fields, (out, act, held, sems) = refs[:n], refs[n:]
    copies = start_copies(fields, held, sems)
    one = jnp.ones((8, LANES), F32)
    m = jnp.full((8, LANES), mass[0], F32)
    m2 = Pair(m * m, jnp.zeros_like(one))
    leaves = [
        jnp.broadcast_to(state[i : i + 1], (8, LANES)) for i in range(tree.num_leaves)
    ]
    s, powers = jax.tree_util.tree_unflatten(tree, leaves)
    s = run_steps(STEP, summed_moments(gathered[...]), s, m2, one, shifts[...], True)
    weights = residues[...]
    c = [
        jnp.broadcast_to(
            jnp.sum(weights * s["sol"][j], axis=1, keepdims=True), (8, LANES)
        )
        for j in range(2 * STEP)
    ]
    t = None
    for j in range(STEP):
        t = plus(t, c[j] * powers[j])
    act[...] = t
    c = [v if j % 2 == 0 else -v for j, v in enumerate(c)]
    for copy in copies:
        copy.wait()
    for k in range(6):
        t = None
        for j in range(2 * STEP):
            t = plus(t, c[j] * held[j, k])
        out[k] = t


def both_ways(x_up, x_down, axis):
    n = lax.axis_size(axis)
    up = [(i, (i + 1) % n) for i in range(n)]
    return lax.ppermute(x_up, axis, up), lax.ppermute(x_down, axis, [(b, a) for a, b in up])


def across(x, step):
    n = lax.axis_size(ZT)
    pairs = [
        (g * n + i, (1 - g) * n + (i + step) % n) for g in range(2) for i in range(n)
    ]
    return lax.ppermute(x, ("grp",) + ZT, pairs)


def everyone(row):
    row = row + lax.ppermute(row, "xy_1", [(0, 1), (1, 0)])
    n = lax.axis_size(REDUCE)
    rows = lax.all_to_all(jnp.broadcast_to(row[None], (n, 1, LANES)), REDUCE, 0, 0, tiled=True)
    rows = rows.reshape(n, LANES)
    return jnp.pad(rows, ((0, -n % 8), (0, 0)))


def field_scratch():
    return [pltpu.VMEM((6, n, ROWS, LANES), F32) for n in (6, 4, 2)]


def held_scratch(n):
    return [pltpu.VMEM((n, *LOCAL), F32), pltpu.SemaphoreType.DMA((n,))]


def state_shape():
    s = jax.ShapeDtypeStruct((8, LANES), F32)
    moments = [Pair(s, s)] * (2 * STEP)
    out = jax.eval_shape(first_state, moments, Pair(s, s), s)
    return jax.tree_util.tree_flatten((out, [s] * STEP))


def on_device(source, links, shifts, residues, mass):
    grp = lax.axis_index("grp")
    place, n_t = lax.axis_index(ZT), lax.axis_size(ZT)
    edges = [(place - 1) % n_t, place, (place + 1) % n_t]
    where = jnp.stack([grp] + [(e == n_t - 1).astype(jnp.int32) for e in edges])
    lane_shifts = jnp.broadcast_to(
        jnp.pad(shifts, (0, LANES - shifts.shape[0]), constant_values=1.0), (8, LANES)
    )
    lane_residues = jnp.broadcast_to(
        jnp.pad(residues, (0, LANES - residues.shape[0])), (8, LANES)
    )
    mine = links.reshape(36, 8, LANES)
    start = source.reshape(LOCAL)
    both = jnp.concatenate([mine, start])
    low, high = both_ways(both, both, ZT)
    wide, up, down = call(
        wide_links_kernel,
        "wide_links",
        [(78, 2, ROWS, LANES), (UP_N, 8, LANES), (DOWN_N, 8, LANES)],
        (where, both, low, high, across(mine, 0), across(mine, 1), across(mine, -1)),
        1,
    )
    low, high = both_ways(up, down, XY)
    ahead_shape, row8, row1 = (12, 8, LANES), (8, LANES), (1, LANES)
    ahead, f1, f2, m, *w = call(
        first_hops_kernel,
        "first_hops",
        [ahead_shape, LOCAL, LOCAL, row8, (18, 5, ROWS, LANES)] + [(18, 4, ROWS, LANES)] * 3,
        (wide, low, high),
        scratch=field_scratch(),
    )

    def hops(field, m, j, kind):
        low, high = both_ways(field, field, XY)
        outs = {
            "wide": [ahead_shape, LOCAL, LOCAL, row8],
            "next": [LOCAL, LOCAL, row1 if j + 1 == 2 * STEP else row8],
            "last": [row1],
        }[kind]
        body = functools.partial(hops_kernel, j, kind)
        return call(
            body, "hops", outs, (field, low, high, m, *w), scratch=field_scratch()
        )

    def taller(field):
        low, high = both_ways(field, field, ZT)
        return call(wide_field_kernel, "wide_field", [(18, 8, LANES)], (field, low, high))[0]

    f3, f4, m = hops(ahead, m, 3, "next")
    ahead, f5, f6, m = hops(taller(f4), m, 5, "wide")
    f7, f8, row = hops(ahead, m, 7, "next")
    gathered = everyone(row)
    ahead, f9, f10, m = hops(taller(f8), m, 9, "wide")
    f11, f12, _ = hops(ahead, m, 11, "next")
    leaves, tree = state_shape()
    count = -(-len(leaves) // 8) * 8
    chain = (start, f1, f2, f3, f4, f5, f6, f7, f8, f9, f10, f11, f12)
    r0, r2, r4, m, state = call(
        restart_kernel,
        "restart",
        [LOCAL, LOCAL, LOCAL, row8, (count, LANES)],
        (mass, gathered, lane_shifts, *chain),
        1,
        len(chain),
        held_scratch(len(chain)),
    )
    ahead, _, r6, m = hops(taller(r4), m, 5, "wide")
    (row,) = hops(ahead, m, 7, "last")
    basis = (start, f2, f4, f6, r0, r2, r4, r6)
    rational, act = call(
        functools.partial(finish_kernel, tree),
        "finish",
        [LOCAL, row8],
        (mass, everyone(row), lane_shifts, lane_residues, state, *basis),
        1,
        len(basis),
        held_scratch(len(basis)),
    )
    act = act[0:1]
    total = act + lax.ppermute(act, "grp", [(0, 1), (1, 0)])
    sites = source.shape[3] * lax.axis_size(XY) * source.shape[4] * n_t * LANES
    sites *= source.shape[0] * lax.axis_size("grp")
    return (rational.reshape(source.shape), (total / sites)[0, 0:1])


def solution(mesh):
    if mesh.size == 512:
        shape = (mesh.shape["grp"], 4, 4, 8, 2)
    else:
        shape = (mesh.shape["grp"], mesh.shape["zt"], 1, mesh.shape["xy"] // 2, 2)
    torus = Mesh(mesh.devices.reshape(shape), ("grp", "zt_0", "zt_1", "xy_0", "xy_1"))
    placed = (
        P("grp", None, None, XY, ZT, None),
        P("grp", None, None, None, XY, ZT, None),
        P(),
        P(),
        P(),
    )
    return jax.shard_map(
        on_device,
        mesh=torus,
        in_specs=placed,
        out_specs=(P("grp", None, None, XY, ZT, None), P()),
        check_vma=False,
    )
```

```python
import functools

import jax
import jax.numpy as jnp
from jax import lax
from jax.experimental import pallas as pl
from jax.experimental.pallas import tpu as pltpu
from jax.sharding import Mesh
from jax.sharding import PartitionSpec as P


NY = 2
NZ = 64
LANES = NY * NZ
STEP = 4
XY = ("xy_0", "xy_1")
ZT = ("zt_0", "zt_1")
F32 = jnp.float32
ROWS = 16
REDUCE = ("zt_0", "zt_1", "xy_0")
LOCAL = (6, 8, LANES)


def two_sum(a, b):
    s = a + b
    t = s - a
    return s, (a - (s - t)) + (b - t)


def quick_sum(a, b):
    s = a + b
    return s, b - (s - a)


def halves(a):
    t = a * 4097.0
    h = t - (t - a)
    return h, a - h


def two_prod(a, b):
    p = a * b
    ah, al = halves(a)
    bh, bl = halves(b)
    return p, ((ah * bh - p) + ah * bl + al * bh) + al * bl


@jax.tree_util.register_pytree_node_class
class Pair:
    def __init__(self, h, l):
        self.h = h
        self.l = l

    def tree_flatten(self):
        return (self.h, self.l), None

    @classmethod
    def tree_unflatten(cls, _, leaves):
        return cls(*leaves)

    def __add__(self, o):
        a, e = two_sum(self.h, o.h)
        t, f = two_sum(self.l, o.l)
        a, e = quick_sum(a, e + t)
        return Pair(*quick_sum(a, e + f))

    def __neg__(self):
        return Pair(-self.h, -self.l)

    def __sub__(self, o):
        return self + (-o)

    def __mul__(self, o):
        p, e = two_prod(self.h, o.h)
        return Pair(*quick_sum(p, e + (self.h * o.l + self.l * o.h)))

    def times(self, f):
        p, e = two_prod(self.h, f)
        return Pair(*quick_sum(p, e + self.l * f))

    def __truediv__(self, o):
        q1 = self.h / o.h
        r = self - o.times(q1)
        q2 = r.h / o.h
        r = r - o.times(q2)
        a, b = quick_sum(q1, q2)
        return Pair(*quick_sum(a, b + r.h / o.h))


def plus(a, b):
    return b if a is None else a + b


def run_steps(first, moments, state, m2, one, shifts, final):
    size = STEP
    al, be, c, gam = (dict(state[n]) for n in ("al", "be", "c", "gam"))
    coef = dict(state["coef"])
    part, sol = dict(state["part"]), dict(state["sol"])
    zeta, zeta_old, zeta_new = state["zeta"], state["zeta_old"], state["zeta_new"]
    unit = Pair(one, jnp.zeros_like(one))
    table = {first: list(moments)}
    raised = {}
    if first:
        inv, own, low = {}, {}, {}
        for k in range(first):
            inv[k] = unit / al[k]
            own[k] = (unit + c[k] if k else unit) * inv[k] - m2
            if k:
                low[k] = c[k] * inv[k]
            table[k] = [None] * (2 * size)
        for i in range(1, 2 * size):
            for k in range(first - 1, -1, -1):
                if i < first - k:
                    continue
                t = None
                if table[k][i - 1] is not None:
                    t = plus(t, own[k] * table[k][i - 1])
                if table[k + 1][i - 1] is not None:
                    t = plus(t, -(inv[k] * table[k + 1][i - 1]))
                if k and table[k - 1][i - 1] is not None:
                    t = plus(t, -(low[k] * table[k - 1][i - 1]))
                table[k][i] = t
        rest, top = state["handover"]
        scale = one / top
        for k in range(first - 1):
            raised[k] = {k + 1: one}
        raised[first - 1] = {j: -(rest[j] * scale) for j in rest}
        raised[first - 1][first] = scale
    for i in range(size - 1):
        raised[first + i] = {first + i + 1: one}
    coef[first] = {first: one}
    lead, second = unit, None
    handover = None
    for d in range(size):
        k = first + d
        norm = lead * table[k][d]
        high = lead * table[k][d + 1]
        if second is not None:
            high = high + second * table[k][d]
        gam[k] = norm
        if k == 0:
            part = {0: jnp.ones_like(shifts)}
        else:
            ratio = norm / gam[k - 1]
            be[k - 1] = ratio
            step = zeta_new / zeta
            keep = ratio.h * step * step
            grown = {}
            for j in sorted(set(part) | set(coef[k])):
                t = None
                if j in coef[k]:
                    t = zeta_new * coef[k][j]
                if j in part:
                    t = plus(t, keep * part[j])
                grown[j] = t
            part = grown
            zeta_old, zeta = zeta, zeta_new
        curve = m2 * norm + high
        if k:
            curve = curve - ratio * norm / al[k - 1]
        a = norm / curve
        al[k] = a
        if k:
            a_old, b_old = al[k - 1].h, be[k - 1].h
            zeta_new = (
                zeta
                * zeta_old
                * a_old
                / (a.h * b_old * (zeta_old - zeta) + zeta_old * a_old * (1.0 + shifts * a.h))
            )
            c[k] = a * be[k - 1] / al[k - 1]
            keep_r = unit + c[k]
        else:
            zeta_new = zeta / (1.0 + shifts * a.h)
            keep_r = unit
        gain = a.h * zeta_new / zeta
        for j in part:
            sol[j] = plus(sol.get(j), gain * part[j])
        if d == size - 1 and final:
            break
        image = {}
        for j, v in coef[k].items():
            image[j] = plus(image.get(j), m2.h * v)
            if j == first + size - 1:
                continue
            for jj, w in raised[j].items():
                image[jj] = plus(image.get(jj), w * v)
        following = {}
        for j in sorted(set(coef[k]) | set(image) | set(coef.get(k - 1, {}))):
            t = None
            if j in coef[k]:
                t = keep_r.h * coef[k][j]
            if j in image:
                t = plus(t, -(a.h * image[j]))
            if k and j in coef[k - 1]:
                t = plus(t, -(c[k].h * coef[k - 1][j]))
            following[j] = t
        if d == size - 1:
            handover = (following, -(a.h * coef[k][first + size - 1]))
            break
        coef[k + 1] = following
        row = [None] * (2 * size)
        for i in range(2 * size - 1 - d):
            if table[k][i] is None or table[k][i + 1] is None:
                continue
            t = keep_r * table[k][i] - a * (m2 * table[k][i] + table[k][i + 1])
            if k and table[k - 1][i] is not None:
                t = t - c[k] * table[k - 1][i]
            row[i] = t
        table[k + 1] = row
        image_second = m2 * lead if second is None else m2 * lead + second
        lead, second = -(a * lead), keep_r * lead - a * image_second
    last = first + size - 1
    return {
        "al": al,
        "be": be,
        "c": c,
        "gam": {last: gam[last]},
        "coef": {last: coef[last]},
        "part": part,
        "sol": sol,
        "zeta": zeta,
        "zeta_old": zeta_old,
        "zeta_new": zeta_new,
        "handover": handover,
    }


def start_state(one):
    return {
        "al": {},
        "be": {},
        "c": {},
        "gam": {},
        "coef": {},
        "part": {},
        "sol": {},
        "zeta": one,
        "zeta_old": one,
        "zeta_new": one,
        "handover": None,
    }


def first_state(moments, m2, shifts):
    one = jnp.ones_like(shifts)
    return run_steps(0, moments, start_state(one), m2, one, shifts, False)


def summed_moments(gathered):
    rows = gathered.shape[0] // 8
    zero = jnp.zeros((8, LANES), F32)
    terms = [Pair(gathered[8 * i : 8 * i + 8], zero) for i in range(rows)]
    while len(terms) > 1:
        terms = [terms[i] + terms[i + 1] for i in range(0, len(terms) - 1, 2)] + (
            [terms[-1]] if len(terms) % 2 else []
        )
    t = terms[0]
    for s in (4, 2, 1):
        t = t + Pair(pltpu.roll(t.h, s, 0), pltpu.roll(t.l, s, 0))
    width = LANES // (2 * STEP)
    s = width // 2
    while s:
        t = t + Pair(pltpu.roll(t.h, LANES - s, 1), pltpu.roll(t.l, LANES - s, 1))
        s //= 2
    lane = lax.broadcasted_iota(jnp.int32, (8, LANES), 1)

    def spread(v, j):
        picked = jnp.where(lane == width * j, v, 0.0)
        return jnp.broadcast_to(jnp.sum(picked, axis=1, keepdims=True), (8, LANES))

    return [Pair(spread(t.h, j), spread(t.l, j)) for j in range(2 * STEP)]


def call(body, outs, args, smem=0, far=0, scratch=()):
    n = len(args)
    specs = [pl.BlockSpec(memory_space=pltpu.SMEM)] * smem
    specs += [pl.BlockSpec(memory_space=pltpu.VMEM)] * (n - smem - far)
    specs += [pl.BlockSpec(memory_space=pl.ANY)] * far
    return pl.pallas_call(
        body,
        in_specs=specs,
        out_specs=[pl.BlockSpec(memory_space=pltpu.VMEM)] * len(outs),
        out_shape=[jax.ShapeDtypeStruct(s, F32) for s in outs],
        scratch_shapes=list(scratch),
        compiler_params=pltpu.CompilerParams(vmem_limit_bytes=12 * 1024 * 1024),
    )(*args)


def wide_links_kernel(where, own, low, high, own_x, low_x, high_x, out, up, down):
    first = where[0] == 0
    flip = [jnp.where(where[i] == 1, -1.0, 1.0).astype(F32) for i in (1, 2, 3)]
    shape = (8, LANES)
    lane = lax.broadcasted_iota(jnp.int32, shape, 1)
    row = lax.broadcasted_iota(jnp.int32, shape, 0)
    x, t = row // 4, row % 4
    y = lane // NZ
    z = lane % NZ
    half = jnp.full(shape, 0.5, F32)
    etas = [
        half,
        jnp.where(x % 2 == 0, half, -half),
        jnp.where((x + y) % 2 == 0, half, -half),
        jnp.where((x + y + z) % 2 == 0, half, -half),
    ]
    zero = jnp.zeros((4, LANES), F32)
    sides = ((low, low_x), (own, own_x), (high, high_x))

    def place(k, parts):
        for i in range(2):
            cut = [v[4 * i : 4 * i + 4] for v in parts]
            out[k, i, 0:4] = cut[0]
            out[k, i, 4:8] = cut[1]
            out[k, i, 8:12] = cut[2]
            out[k, i, 12:16] = zero

    for mu in range(4):
        signs = [
            jnp.where(t == 3, etas[mu] * flip[i], etas[mu]) if mu == 3 else etas[mu]
            for i in range(3)
        ]

        def one(k, _, mu=mu, signs=signs):
            j = 18 * (mu % 2) + k
            parts = []
            for (a, b), s in zip(sides, signs):
                mine, theirs = a[j], b[j]
                w = jnp.where(first, mine, theirs) if mu < 2 else jnp.where(first, theirs, mine)
                parts.append(w * s)
            place(18 * mu + k, parts)
            return 0

        lax.fori_loop(0, 18, one, 0)
    for k in range(6):
        place(72 + k, [a[36 + k] for a, _ in sides])

    def pack(k, _):
        for i in range(2):
            up[2 * k + i] = out[2 * k + i, 1, 0:8]
            down[2 * k + i] = out[2 * k + i, 0, 0:8]
            up[102 + k, 4 * i : 4 * i + 4] = out[2 * k + i, 1, 8:12]
            down[84 + k, 4 * i : 4 * i + 4] = out[2 * k + i, 0, 8:12]
        return 0

    lax.fori_loop(0, 36, pack, 0)
    for k in range(9):
        for i in range(2):
            up[72 + 2 * k + i] = out[2 * k + i, 0, 0:8]
            up[138 + k, 4 * i : 4 * i + 4] = out[2 * k + i, 0, 8:12]
    for k in range(6):
        for i in range(2):
            up[90 + 2 * k + i] = out[72 + k, i, 0:8]
            down[72 + 2 * k + i] = out[72 + k, i, 0:8]
            up[147 + k, 4 * i : 4 * i + 4] = out[72 + k, i, 8:12]
            down[120 + k, 4 * i : 4 * i + 4] = out[72 + k, i, 8:12]


UP_N = 153
DOWN_N = 126


def wide_field_kernel(own, low, high, out):
    for f in range(own.shape[0] // 6):
        for k in range(6):
            for x in range(2):
                c, i, o = slice(4 * x, 4 * x + 4), 6 * f + k, 18 * f
                out[o + 2 * k + x, 0:4] = low[i, c]
                out[o + 2 * k + x, 4:8] = own[i, c]
                out[o + 12 + k, c] = high[i, c]


def unpack_wide(v0, ref, own, low, high):
    for k in range(6):
        for x in range(2):
            for i, o in ((0, low), (2, own), (4, high)):
                v0[k, i + x, 0:8] = ref[o + 2 * k + x]
                v0[k, i + x, 8:12] = ref[o + 12 + k, 4 * x : 4 * x + 4]


def z_ahead(v, vy, z):
    return jnp.where(z == NZ - 1, pltpu.roll(vy, LANES - 1, 1), pltpu.roll(v, LANES - 1, 1))


def z_behind(v, vy, z):
    return jnp.where(z == 0, pltpu.roll(vy, 1, 1), pltpu.roll(v, 1, 1))


def times(acc, link, v):
    for r in range(3):
        for c in range(3):
            re, im = link(3 * r + c), link(9 + 3 * r + c)
            acc[r] = acc[r] + re * v[c] - im * v[3 + c]
            acc[3 + r] = acc[3 + r] + re * v[3 + c] + im * v[c]


def adjoint(link, v):
    acc = [None] * 6
    for r in range(3):
        for c in range(3):
            re, im = link(3 * c + r), link(9 + 3 * c + r)
            acc[r] = plus(acc[r], re * v[c] + im * v[3 + c])
            acc[3 + r] = plus(acc[3 + r], re * v[3 + c] - im * v[c])
    return acc


def hop(src, dst, rows, base, links):
    lx, ly, lz, lt = links
    z = lax.broadcasted_iota(jnp.int32, (ROWS, LANES), 1) % NZ

    def one(i, _):
        s = base + i
        v = [src[k, i + 1] for k in range(6)]
        vy = [pltpu.roll(u, NZ, 1) for u in v]
        back = adjoint(lambda k: lz[k, s], v)
        acc = [-z_behind(u, pltpu.roll(u, NZ, 1), z) for u in back]
        times(acc, lambda k: lz[k, s], [z_ahead(u, w, z) for u, w in zip(v, vy)])
        times(acc, lambda k: ly[k, s], vy)
        back = adjoint(lambda k: lt[k, s], v)
        acc = [a - pltpu.roll(u, 1, 0) for a, u in zip(acc, back)]
        times(acc, lambda k: lt[k, s], [pltpu.roll(u, ROWS - 1, 0) for u in v])
        times(acc, lambda k: lx[k, s + 1], [src[k, i + 2] for k in range(6)])
        back = adjoint(lambda k: lx[k, s], [src[k, i] for k in range(6)])
        for k in range(6):
            dst[k, i] = acc[k] - back[k]
        return 0

    lax.fori_loop(0, rows, one, 0)


def own_norm(src, x0):
    t = None
    for k in range(6):
        for x in range(2):
            v = src[k, x0 + x, 4:8]
            t = plus(t, v * v)
    return jnp.sum(t, axis=0, keepdims=True)


def set_row(moments, j, t):
    row = lax.broadcasted_iota(jnp.int32, (8, LANES), 0)
    return jnp.where(row == j, jnp.broadcast_to(t, (8, LANES)), moments)


def message_row(m):
    s = LANES // 2
    while s >= LANES // (2 * STEP):
        m = m + pltpu.roll(m, s, 1)
        s //= 2
    row = lax.broadcasted_iota(jnp.int32, (8, LANES), 0)
    lane = lax.broadcasted_iota(jnp.int32, (8, LANES), 1)
    m = jnp.where(lane // (LANES // (2 * STEP)) == row, m, 0.0)
    return jnp.sum(m, axis=0, keepdims=True)


def two_hops(j, m, v0, v1, v2, links):
    hop(v0, v1, 4, 0, links)
    hop(v1, v2, 2, 1, links)
    m = set_row(m, j, own_norm(v1, 1))
    return set_row(m, j + 1, own_norm(v2, 0)) if j + 1 < 2 * STEP else m


def put_ahead(ahead, v2):
    for k in range(6):
        for x in range(2):
            ahead[2 * k + x] = v2[k, x, 2:10]


def first_hops_kernel(own, low, high, ahead, moments, lx, ly, lz, lt, kept, v0, v1, v2):
    links = (lx, ly, lz, lt)

    def side(msg, i, half):
        def at(k):
            c = 4 * (k % 2)
            return msg[i + k], msg[half + k // 2, slice(c, c + 4)]

        return at

    def store(dst, pieces):
        dst[0:8] = pieces[0]
        dst[8:12] = pieces[1]
        dst[12:16] = jnp.zeros((4, LANES), F32)

    behind, behind2, ahead1 = side(low, 0, 102), side(low, 72, 138), side(high, 0, 84)
    for k in range(18):
        store(lx.at[k, 0], behind2(k))
        store(lx.at[k, 1], behind(k))
        lx[k, 2] = own[k, 0]
        lx[k, 3] = own[k, 1]
        store(lx.at[k, 4], ahead1(k))
        for i, ref in ((36, lz), (54, lt)):
            store(ref.at[k, 0], behind(i + k))
            ref[k, 1] = own[i + k, 0]
            ref[k, 2] = own[i + k, 1]
            store(ref.at[k, 3], ahead1(i + k))
        store(v2.at[0, 0], behind(18 + k))
        store(v2.at[0, 1], ahead1(18 + k))
        c, r = (k % 9) % 3, (k % 9) // 3
        ly[k, 0] = v2[0, 0]
        ly[k, 1] = own[18 + k, 0]
        ly[k, 2] = own[18 + k, 1]
        ly[k, 3] = v2[0, 1]
    for i in range(4):
        for r in range(3):
            for c in range(r + 1):
                k, a = 3 * r + c, 3 * c + r
                u, w = ly[k, i], ly[a, i]
                ur, wr = pltpu.roll(u, NZ, 1), pltpu.roll(w, NZ, 1)
                ly[k, i] = u - wr
                if a != k:
                    ly[a, i] = w - ur
                u, w = ly[9 + k, i], ly[9 + a, i]
                ur, wr = pltpu.roll(u, NZ, 1), pltpu.roll(w, NZ, 1)
                ly[9 + k, i] = u + wr
                if a != k:
                    ly[9 + a, i] = w + ur
    for k in range(6):
        for x in range(2):
            c = slice(4 * x, 4 * x + 4)
            kept[2 * k + x] = own[72 + k, x, 0:8]
            kept[12 + k, c] = own[72 + k, x, 8:12]
    kept[18:30] = low[90:102]
    kept[30:36] = low[147:153]
    kept[36:48] = high[72:84]
    kept[48:54] = high[120:126]
    unpack_wide(v0, kept, 0, 18, 36)
    m = set_row(jnp.zeros((8, LANES), F32), 0, own_norm(v0, 2))
    moments[...] = two_hops(1, m, v0, v1, v2, links)
    put_ahead(ahead, v2)


def hops_kernel(j, kind, own, low, high, before, lx, ly, lz, lt, *rest):
    links = (lx, ly, lz, lt)
    outs, (v0, v1, v2) = rest[:-3], rest[-3:]
    for k in range(6):
        for x in range(2):
            for i, ref in ((0, low), (2, own), (4, high)):
                if kind == "wide":
                    v0[k, i + x, 0:8] = ref[2 * k + x]
                    v0[k, i + x, 8:12] = ref[12 + k, 4 * x : 4 * x + 4]
                else:
                    v0[k, i + x, 2:10] = ref[2 * k + x]
    m = before[...]
    if kind == "last":
        (moments,) = outs
        hop(v0.at[:, 1:5], v2, 2, 1, links)
        moments[...] = message_row(set_row(m, j, own_norm(v2, 0)))
        return
    m = two_hops(j, m, v0, v1, v2, links)
    field, moments = outs
    if kind == "wide":
        put_ahead(field, v2)
    else:
        for k in range(6):
            for x in range(2):
                c = slice(4 * x, 4 * x + 4)
                field[k, c] = v2[k, x, 4:8]
                if field.shape[0] == 12:
                    field[6 + k, c] = own[2 * k + x, 2:6]
    moments[...] = message_row(m) if j + 1 == 2 * STEP else m


def start_copies(fields, held, sems):
    copies = [pltpu.make_async_copy(f, h, sems.at[i]) for i, (f, h) in enumerate(zip(fields, held))]
    for c in copies:
        c.start()
    return copies


def restart_kernel(mass, gathered, shifts, lx, ly, lz, lt, *refs):
    fields, (r0, ahead, moments, state), scratch = refs[:7], refs[7:11], refs[11:]
    held, (sems, sum_, v0, v1, v2) = scratch[:7], scratch[7:]
    copies = start_copies(fields, held, sems)
    one = jnp.ones((8, LANES), F32)
    m = jnp.full((8, LANES), mass[0], F32)
    m2 = Pair(m * m, jnp.zeros_like(one))
    powers = summed_moments(gathered[...])
    s = first_state(powers, m2, shifts[...])
    leaves, _ = jax.tree_util.tree_flatten((s, [p.h for p in powers[:STEP]]))
    for i, leaf in enumerate(leaves):
        state[i : i + 1] = leaf[0:1]
    rest, top = s["handover"]
    c = [rest[0], -rest[1], rest[2], -rest[3], top]
    for copy in copies:
        copy.wait()
    kept, four, eight = held[0], held[1:4], held[4:7]
    for side in range(3):
        a, b, o = four[side], eight[side], 18 * side

        def one_tile(i, _, a=a, b=b, o=o):
            sum_[o + i] = (
                c[0] * kept[o + i]
                + c[1] * a[18 + i]
                + c[2] * a[i]
                + c[3] * b[18 + i]
                + c[4] * b[i]
            )
            return 0

        lax.fori_loop(0, 18, one_tile, 0)
    unpack_wide(v0, sum_, 0, 18, 36)
    for k in range(6):
        for x in range(2):
            r0[k, 4 * x : 4 * x + 4] = v0[k, 2 + x, 4:8]
    m = set_row(jnp.zeros((8, LANES), F32), 0, own_norm(v0, 2))
    moments[...] = two_hops(1, m, v0, v1, v2, (lx, ly, lz, lt))
    put_ahead(ahead, v2)


def finish_kernel(tree, mass, gathered, shifts, residues, state, *refs):
    fields, (out, act), scratch = refs[:7], refs[7:9], refs[9:]
    held, sems = scratch[:7], scratch[7]
    copies = start_copies(fields, held, sems)
    one = jnp.ones((8, LANES), F32)
    m = jnp.full((8, LANES), mass[0], F32)
    m2 = Pair(m * m, jnp.zeros_like(one))
    leaves = [jnp.broadcast_to(state[i : i + 1], (8, LANES)) for i in range(tree.num_leaves)]
    s, powers = jax.tree_util.tree_unflatten(tree, leaves)
    s = run_steps(STEP, summed_moments(gathered[...]), s, m2, one, shifts[...], True)
    weights = residues[...]
    c = [
        jnp.broadcast_to(jnp.sum(weights * s["sol"][j], axis=1, keepdims=True), (8, LANES))
        for j in range(2 * STEP)
    ]
    t = None
    for j in range(STEP):
        t = plus(t, c[j] * powers[j])
    act[...] = t
    c = [(v if j % 2 == 0 else -v)[0:4] for j, v in enumerate(c)]
    for copy in copies:
        copy.wait()
    start, four, eight, r0, r2, r4, r6 = held
    for k in range(6):
        for x in range(2):
            q, i = slice(4 * x, 4 * x + 4), 2 * k + x
            terms = (
                start[k, q],
                four[18 + i, 4:8],
                four[i, 4:8],
                eight[18 + i, 4:8],
                r0[k, q],
                r2[i, 2:6],
                r4[k, q],
                r6[i, 2:6],
            )
            t = None
            for w, v in zip(c, terms):
                t = plus(t, w * v)
            out[k, q] = t


def both_ways(x_up, x_down, axis):
    n = lax.axis_size(axis)
    up = [(i, (i + 1) % n) for i in range(n)]
    return lax.ppermute(x_up, axis, up), lax.ppermute(x_down, axis, [(b, a) for a, b in up])


def across(x, step):
    n = lax.axis_size(ZT)
    pairs = [
        (g * n + i, (1 - g) * n + (i + step) % n) for g in range(2) for i in range(n)
    ]
    return lax.ppermute(x, ("grp",) + ZT, pairs)


def everyone(row, later):
    row = row + lax.ppermute(row, "xy_1", [(0, 1), (1, 0)])
    n = lax.axis_size(REDUCE)
    rows, later = lax.optimization_barrier((jnp.broadcast_to(row[None], (n, 1, LANES)), later))
    rows = lax.all_to_all(rows, REDUCE, 0, 0, tiled=True).reshape(n, LANES)
    return jnp.pad(rows, ((0, -n % 8), (0, 0))), later


def field_scratch():
    return [pltpu.VMEM((6, n, ROWS, LANES), F32) for n in (6, 4, 2)]


def held_scratch(fields):
    return [pltpu.VMEM(f.shape, F32) for f in fields] + [pltpu.SemaphoreType.DMA((len(fields),))]


def state_shape():
    s = jax.ShapeDtypeStruct((8, LANES), F32)
    moments = [Pair(s, s)] * (2 * STEP)
    out = jax.eval_shape(first_state, moments, Pair(s, s), s)
    return jax.tree_util.tree_flatten((out, [s] * STEP))


def on_device(source, links, shifts, residues, mass):
    grp = lax.axis_index("grp")
    place, n_t = lax.axis_index(ZT), lax.axis_size(ZT)
    edges = [(place - 1) % n_t, place, (place + 1) % n_t]
    where = jnp.stack([grp] + [(e == n_t - 1).astype(jnp.int32) for e in edges])
    lane_shifts = jnp.broadcast_to(
        jnp.pad(shifts, (0, LANES - shifts.shape[0]), constant_values=1.0), (8, LANES)
    )
    mine = links.reshape(36, 8, LANES)
    start = source.reshape(LOCAL)
    both = jnp.concatenate([mine, start])
    low, high = both_ways(both, both, ZT)
    wide, up, down = call(
        wide_links_kernel,
        [(78, 2, ROWS, LANES), (UP_N, 8, LANES), (DOWN_N, 8, LANES)],
        (where, both, low, high, across(mine, 0), across(mine, 1), across(mine, -1)),
        1,
    )
    low, high = both_ways(up, down, XY)
    ahead_shape, row8, row1 = (12, 8, LANES), (8, LANES), (1, LANES)
    ahead, m, *rest = call(
        first_hops_kernel,
        [ahead_shape, row8, (18, 5, ROWS, LANES)]
        + [(18, 4, ROWS, LANES)] * 3
        + [(54, 8, LANES)],
        (wide, low, high),
        scratch=field_scratch(),
    )
    w, kept = rest[:4], rest[4]

    def hops(own, low, high, m, j, kind, fields=1):
        outs = {
            "wide": [ahead_shape, row8],
            "next": [(6 * fields, 8, LANES), row1 if j + 1 == 2 * STEP else row8],
            "last": [row1],
        }[kind]
        body = functools.partial(hops_kernel, j, kind)
        return call(body, outs, (own, low, high, m, *w), scratch=field_scratch())

    def around(field):
        return (field, *both_ways(field, field, XY))

    def tall(field, low, high):
        shape = (3 * field.shape[0], 8, LANES)
        return call(wide_field_kernel, [shape], (field, low, high))[0]

    def taller(field):
        return tall(field, *both_ways(field, field, ZT))

    f4, m = hops(*around(ahead), m, 3, "next", 2)
    four = around(taller(f4))
    ahead, m = hops(*four, m, 5, "wide")
    f8, row = hops(*around(ahead), m, 7, "next", 2)
    gathered, f8 = everyone(row, f8)
    low, high = both_ways(f8, f8, ZT)
    eight = around(tall(f8, low, high))
    leaves, tree = state_shape()
    count = -(-len(leaves) // 8) * 8
    fields = (kept, *four, *eight)
    r0, r2, m, state = call(
        restart_kernel,
        [LOCAL, ahead_shape, row8, (count, LANES)],
        (mass, gathered, lane_shifts, *w, *fields),
        1,
        len(fields),
        held_scratch(fields) + [pltpu.VMEM((54, 8, LANES), F32)] + field_scratch(),
    )
    r4, m = hops(*around(r2), m, 3, "next")
    r6, m = hops(*around(taller(r4)), m, 5, "wide")
    (row,) = hops(*around(r6), m, 7, "last")
    lane_residues = jnp.broadcast_to(
        jnp.pad(residues, (0, LANES - residues.shape[0])), (8, LANES)
    )
    gathered, lane_residues = everyone(row, lane_residues)
    fields = (start, four[0], eight[0], r0, r2, r4, r6)
    rational, act = call(
        functools.partial(finish_kernel, tree),
        [LOCAL, row8],
        (mass, gathered, lane_shifts, lane_residues, state, *fields),
        1,
        len(fields),
        held_scratch(fields),
    )
    act = act[0:1]
    total = act + lax.ppermute(act, "grp", [(0, 1), (1, 0)])
    sites = source.shape[3] * lax.axis_size(XY) * source.shape[4] * n_t * LANES
    sites *= source.shape[0] * lax.axis_size("grp")
    return (rational.reshape(source.shape), (total / sites)[0, 0:1])


def solution(mesh):
    if mesh.size == 512:
        shape = (mesh.shape["grp"], 4, 4, 8, 2)
    else:
        shape = (mesh.shape["grp"], mesh.shape["zt"], 1, mesh.shape["xy"] // 2, 2)
    torus = Mesh(mesh.devices.reshape(shape), ("grp", "zt_0", "zt_1", "xy_0", "xy_1"))
    placed = (
        P("grp", None, None, XY, ZT, None),
        P("grp", None, None, None, XY, ZT, None),
        P(),
        P(),
        P(),
    )
    step = jax.shard_map(
        on_device,
        mesh=torus,
        in_specs=placed,
        out_specs=(P("grp", None, None, XY, ZT, None), P()),
        check_vma=False,
    )
    if mesh.size != 512:
        return step
    return step
```

```python
import functools

import jax
import jax.numpy as jnp
from jax import lax
from jax.experimental import pallas as pl
from jax.experimental.pallas import tpu as pltpu
from jax.sharding import Mesh
from jax.sharding import PartitionSpec as P


NY = 2
NZ = 64
LANES = NY * NZ
STEP = 4
XY = ("xy_0", "xy_1")
ZT = ("zt_0", "zt_1")
F32 = jnp.float32
ROWS = 16
UNROLL = True
REDUCE = ("zt_0", "zt_1", "xy_0")
LOCAL = (6, 8, LANES)


def two_sum(a, b):
    s = a + b
    t = s - a
    return s, (a - (s - t)) + (b - t)


def quick_sum(a, b):
    s = a + b
    return s, b - (s - a)


def halves(a):
    t = a * 4097.0
    h = t - (t - a)
    return h, a - h


def two_prod(a, b):
    p = a * b
    ah, al = halves(a)
    bh, bl = halves(b)
    return p, ((ah * bh - p) + ah * bl + al * bh) + al * bl


@jax.tree_util.register_pytree_node_class
class Pair:
    def __init__(self, h, l):
        self.h = h
        self.l = l

    def tree_flatten(self):
        return (self.h, self.l), None

    @classmethod
    def tree_unflatten(cls, _, leaves):
        return cls(*leaves)

    def __add__(self, o):
        a, e = two_sum(self.h, o.h)
        t, f = two_sum(self.l, o.l)
        a, e = quick_sum(a, e + t)
        return Pair(*quick_sum(a, e + f))

    def __neg__(self):
        return Pair(-self.h, -self.l)

    def __sub__(self, o):
        return self + (-o)

    def __mul__(self, o):
        p, e = two_prod(self.h, o.h)
        return Pair(*quick_sum(p, e + (self.h * o.l + self.l * o.h)))

    def times(self, f):
        p, e = two_prod(self.h, f)
        return Pair(*quick_sum(p, e + self.l * f))

    def __truediv__(self, o):
        q1 = self.h / o.h
        r = self - o.times(q1)
        q2 = r.h / o.h
        r = r - o.times(q2)
        a, b = quick_sum(q1, q2)
        return Pair(*quick_sum(a, b + r.h / o.h))


def plus(a, b):
    return b if a is None else a + b


def run_steps(first, moments, state, m2, one, shifts, final):
    size = STEP
    al, be, c, gam = (dict(state[n]) for n in ("al", "be", "c", "gam"))
    coef = dict(state["coef"])
    part, sol = dict(state["part"]), dict(state["sol"])
    zeta, zeta_old, zeta_new = state["zeta"], state["zeta_old"], state["zeta_new"]
    unit = Pair(one, jnp.zeros_like(one))
    table = {first: list(moments)}
    raised = {}
    if first:
        inv, own, low = {}, {}, {}
        for k in range(first):
            inv[k] = unit / al[k]
            own[k] = (unit + c[k] if k else unit) * inv[k] - m2
            if k:
                low[k] = c[k] * inv[k]
            table[k] = [None] * (2 * size)
        for i in range(1, 2 * size):
            for k in range(first - 1, -1, -1):
                if i < first - k:
                    continue
                t = None
                if table[k][i - 1] is not None:
                    t = plus(t, own[k] * table[k][i - 1])
                if table[k + 1][i - 1] is not None:
                    t = plus(t, -(inv[k] * table[k + 1][i - 1]))
                if k and table[k - 1][i - 1] is not None:
                    t = plus(t, -(low[k] * table[k - 1][i - 1]))
                table[k][i] = t
        rest, top = state["handover"]
        scale = one / top
        for k in range(first - 1):
            raised[k] = {k + 1: one}
        raised[first - 1] = {j: -(rest[j] * scale) for j in rest}
        raised[first - 1][first] = scale
    for i in range(size - 1):
        raised[first + i] = {first + i + 1: one}
    coef[first] = {first: one}
    lead, second = unit, None
    handover = None
    for d in range(size):
        k = first + d
        norm = lead * table[k][d]
        high = lead * table[k][d + 1]
        if second is not None:
            high = high + second * table[k][d]
        gam[k] = norm
        if k == 0:
            part = {0: jnp.ones_like(shifts)}
        else:
            ratio = norm / gam[k - 1]
            be[k - 1] = ratio
            step = zeta_new / zeta
            keep = ratio.h * step * step
            grown = {}
            for j in sorted(set(part) | set(coef[k])):
                t = None
                if j in coef[k]:
                    t = zeta_new * coef[k][j]
                if j in part:
                    t = plus(t, keep * part[j])
                grown[j] = t
            part = grown
            zeta_old, zeta = zeta, zeta_new
        curve = m2 * norm + high
        if k:
            curve = curve - ratio * norm / al[k - 1]
        a = norm / curve
        al[k] = a
        if k:
            a_old, b_old = al[k - 1].h, be[k - 1].h
            zeta_new = (
                zeta
                * zeta_old
                * a_old
                / (a.h * b_old * (zeta_old - zeta) + zeta_old * a_old * (1.0 + shifts * a.h))
            )
            c[k] = a * be[k - 1] / al[k - 1]
            keep_r = unit + c[k]
        else:
            zeta_new = zeta / (1.0 + shifts * a.h)
            keep_r = unit
        gain = a.h * zeta_new / zeta
        for j in part:
            sol[j] = plus(sol.get(j), gain * part[j])
        if d == size - 1 and final:
            break
        image = {}
        for j, v in coef[k].items():
            image[j] = plus(image.get(j), m2.h * v)
            if j == first + size - 1:
                continue
            for jj, w in raised[j].items():
                image[jj] = plus(image.get(jj), w * v)
        following = {}
        for j in sorted(set(coef[k]) | set(image) | set(coef.get(k - 1, {}))):
            t = None
            if j in coef[k]:
                t = keep_r.h * coef[k][j]
            if j in image:
                t = plus(t, -(a.h * image[j]))
            if k and j in coef[k - 1]:
                t = plus(t, -(c[k].h * coef[k - 1][j]))
            following[j] = t
        if d == size - 1:
            handover = (following, -(a.h * coef[k][first + size - 1]))
            break
        coef[k + 1] = following
        row = [None] * (2 * size)
        for i in range(2 * size - 1 - d):
            if table[k][i] is None or table[k][i + 1] is None:
                continue
            t = keep_r * table[k][i] - a * (m2 * table[k][i] + table[k][i + 1])
            if k and table[k - 1][i] is not None:
                t = t - c[k] * table[k - 1][i]
            row[i] = t
        table[k + 1] = row
        image_second = m2 * lead if second is None else m2 * lead + second
        lead, second = -(a * lead), keep_r * lead - a * image_second
    last = first + size - 1
    return {
        "al": al,
        "be": be,
        "c": c,
        "gam": {last: gam[last]},
        "coef": {last: coef[last]},
        "part": part,
        "sol": sol,
        "zeta": zeta,
        "zeta_old": zeta_old,
        "zeta_new": zeta_new,
        "handover": handover,
    }


def start_state(one):
    return {
        "al": {},
        "be": {},
        "c": {},
        "gam": {},
        "coef": {},
        "part": {},
        "sol": {},
        "zeta": one,
        "zeta_old": one,
        "zeta_new": one,
        "handover": None,
    }


def first_state(moments, m2, shifts):
    one = jnp.ones_like(shifts)
    return run_steps(0, moments, start_state(one), m2, one, shifts, False)


def summed_moments(gathered):
    rows = gathered.shape[0] // 8
    zero = jnp.zeros((8, LANES), F32)
    terms = [Pair(gathered[8 * i : 8 * i + 8], zero) for i in range(rows)]
    while len(terms) > 1:
        terms = [terms[i] + terms[i + 1] for i in range(0, len(terms) - 1, 2)] + (
            [terms[-1]] if len(terms) % 2 else []
        )
    t = terms[0]
    for s in (4, 2, 1):
        t = t + Pair(pltpu.roll(t.h, s, 0), pltpu.roll(t.l, s, 0))
    width = LANES // (2 * STEP)
    s = width // 2
    while s:
        t = t + Pair(pltpu.roll(t.h, LANES - s, 1), pltpu.roll(t.l, LANES - s, 1))
        s //= 2
    lane = lax.broadcasted_iota(jnp.int32, (8, LANES), 1)

    def spread(v, j):
        picked = jnp.where(lane == width * j, v, 0.0)
        return jnp.broadcast_to(jnp.sum(picked, axis=1, keepdims=True), (8, LANES))

    return [Pair(spread(t.h, j), spread(t.l, j)) for j in range(2 * STEP)]


def call(body, outs, args, smem=0, far=0, scratch=()):
    n = len(args)
    specs = [pl.BlockSpec(memory_space=pltpu.SMEM)] * smem
    specs += [pl.BlockSpec(memory_space=pltpu.VMEM)] * (n - smem - far)
    specs += [pl.BlockSpec(memory_space=pl.ANY)] * far
    return pl.pallas_call(
        body,
        in_specs=specs,
        out_specs=[pl.BlockSpec(memory_space=pltpu.VMEM)] * len(outs),
        out_shape=[jax.ShapeDtypeStruct(s, F32) for s in outs],
        scratch_shapes=list(scratch),
        compiler_params=pltpu.CompilerParams(vmem_limit_bytes=12 * 1024 * 1024),
    )(*args)


def rim(dst, k, x, row):
    dst[k, 4 * x : 4 * x + 2] = row[8:10]
    dst[k, 4 * x + 2 : 4 * x + 4] = row[14:16]


def from_rim(dst, half):
    dst[8:10] = half[0:2]
    dst[14:16] = half[2:4]


def wide_links_kernel(where, own, low, high, own_x, low_x, high_x, out, up, down):
    first = where[0] == 0
    flip = [jnp.where(where[i] == 1, -1.0, 1.0).astype(F32) for i in (1, 2, 3)]
    shape = (8, LANES)
    lane = lax.broadcasted_iota(jnp.int32, shape, 1)
    row = lax.broadcasted_iota(jnp.int32, shape, 0)
    x, t = row // 4, row % 4
    y = lane // NZ
    z = lane % NZ
    half = jnp.full(shape, 0.5, F32)
    etas = [
        half,
        jnp.where(x % 2 == 0, half, -half),
        jnp.where((x + y) % 2 == 0, half, -half),
        jnp.where((x + y + z) % 2 == 0, half, -half),
    ]
    zero = jnp.zeros((4, LANES), F32)
    sides = ((low, low_x), (own, own_x), (high, high_x))

    def place(k, parts):
        for i in range(2):
            cut = [v[4 * i : 4 * i + 4] for v in parts]
            out[k, i, 0:2] = cut[0][2:4]
            out[k, i, 2:6] = cut[1]
            out[k, i, 6:10] = cut[2]
            out[k, i, 10:14] = zero
            out[k, i, 14:16] = cut[0][0:2]

    for mu in range(4):
        signs = [
            jnp.where(t == 3, etas[mu] * flip[i], etas[mu]) if mu == 3 else etas[mu]
            for i in range(3)
        ]

        def one(k, _, mu=mu, signs=signs):
            j = 18 * (mu % 2) + k
            parts = []
            for (a, b), s in zip(sides, signs):
                mine, theirs = a[j], b[j]
                w = jnp.where(first, mine, theirs) if mu < 2 else jnp.where(first, theirs, mine)
                parts.append(w * s)
            place(18 * mu + k, parts)
            return 0

        lax.fori_loop(0, 18, one, 0)
    for k in range(6):
        place(72 + k, [a[36 + k] for a, _ in sides])

    def pack(k, _):
        for i in range(2):
            up[2 * k + i] = out[2 * k + i, 1, 0:8]
            down[2 * k + i] = out[2 * k + i, 0, 0:8]
            rim(up, 102 + k, i, out[2 * k + i, 1])
            rim(down, 84 + k, i, out[2 * k + i, 0])
        return 0

    lax.fori_loop(0, 36, pack, 0)
    for k in range(9):
        for i in range(2):
            up[72 + 2 * k + i] = out[2 * k + i, 0, 0:8]
            rim(up, 138 + k, i, out[2 * k + i, 0])
    for k in range(6):
        for i in range(2):
            up[90 + 2 * k + i] = out[72 + k, i, 0:8]
            down[72 + 2 * k + i] = out[72 + k, i, 0:8]
            rim(up, 147 + k, i, out[72 + k, i])
            rim(down, 120 + k, i, out[72 + k, i])


UP_N = 153
DOWN_N = 126


def wide_field_kernel(own, low, high, out):
    for f in range(own.shape[0] // 6):
        for k in range(6):
            for x in range(2):
                c, i, o = slice(4 * x, 4 * x + 4), 6 * f + k, 18 * f
                back, ahead = low[i, c], high[i, c]
                out[o + 2 * k + x, 0:2] = back[2:4]
                out[o + 2 * k + x, 2:6] = own[i, c]
                out[o + 2 * k + x, 6:8] = ahead[0:2]
                out[o + 12 + k, 4 * x : 4 * x + 2] = ahead[2:4]
                out[o + 12 + k, 4 * x + 2 : 4 * x + 4] = back[0:2]


def unpack_wide(v0, ref, own, low, high):
    for k in range(6):
        for x in range(2):
            for i, o in ((0, low), (2, own), (4, high)):
                v0[k, i + x, 0:8] = ref[o + 2 * k + x]
                from_rim(v0.at[k, i + x], ref[o + 12 + k, 4 * x : 4 * x + 4])


def z_ahead(v, vy, z):
    return jnp.where(z == NZ - 1, pltpu.roll(vy, LANES - 1, 1), pltpu.roll(v, LANES - 1, 1))


def z_behind(v, vy, z):
    return jnp.where(z == 0, pltpu.roll(vy, 1, 1), pltpu.roll(v, 1, 1))


def times(acc, link, v):
    for r in range(3):
        for c in range(3):
            re, im = link(3 * r + c), link(9 + 3 * r + c)
            acc[r] = acc[r] + re * v[c] - im * v[3 + c]
            acc[3 + r] = acc[3 + r] + re * v[3 + c] + im * v[c]


def less_adjoint(acc, link, v):
    for r in range(3):
        for c in range(3):
            re, im = link(3 * c + r), link(9 + 3 * c + r)
            acc[r] = acc[r] - re * v[c] - im * v[3 + c]
            acc[3 + r] = acc[3 + r] - re * v[3 + c] + im * v[c]


def adjoint(link, v):
    acc = [None] * 6
    for r in range(3):
        for c in range(3):
            re, im = link(3 * c + r), link(9 + 3 * c + r)
            acc[r] = plus(acc[r], re * v[c] + im * v[3 + c])
            acc[3 + r] = plus(acc[3 + r], re * v[3 + c] - im * v[c])
    return acc


def hop(src, dst, rows, base, links):
    lx, ly, lz, lt, ltb = links
    tall, n = src.shape[2], dst.shape[2]
    z = lax.broadcasted_iota(jnp.int32, (n, LANES), 1) % NZ

    def part(ref):
        return lambda k, i: ref[k, i, 0:n]

    gx, gy, gz, gt, gtb, field = (part(r) for r in (lx, ly, lz, lt, ltb, src))

    def one(i, _):
        s = base + i
        v = [field(k, i + 1) for k in range(6)]
        vy = [pltpu.roll(u, NZ, 1) for u in v]
        back = adjoint(lambda k: gz(k, s), v)
        acc = [-z_behind(u, pltpu.roll(u, NZ, 1), z) for u in back]
        times(acc, lambda k: gz(k, s), [z_ahead(u, w, z) for u, w in zip(v, vy)])
        times(acc, lambda k: gy(k, s), vy)
        whole = [src[k, i + 1] for k in range(6)]
        times(acc, lambda k: gt(k, s), [pltpu.roll(u, tall - 1, 0)[0:n] for u in whole])
        less_adjoint(acc, lambda k: gtb(k, s), [pltpu.roll(u, 1, 0)[0:n] for u in whole])
        times(acc, lambda k: gx(k, s + 1), [field(k, i + 2) for k in range(6)])
        less_adjoint(acc, lambda k: gx(k, s), [field(k, i) for k in range(6)])
        for k in range(6):
            dst[k, i] = acc[k]
        return 0

    lax.fori_loop(0, rows, one, 0, unroll=UNROLL)


def own_norm(src, x0):
    t = None
    for k in range(6):
        for x in range(2):
            v = src[k, x0 + x, 2:6]
            t = plus(t, v * v)
    return jnp.sum(t, axis=0, keepdims=True)


def set_row(moments, j, t):
    row = lax.broadcasted_iota(jnp.int32, (8, LANES), 0)
    return jnp.where(row == j, jnp.broadcast_to(t, (8, LANES)), moments)


def message_row(m):
    s = LANES // 2
    while s >= LANES // (2 * STEP):
        m = m + pltpu.roll(m, s, 1)
        s //= 2
    row = lax.broadcasted_iota(jnp.int32, (8, LANES), 0)
    lane = lax.broadcasted_iota(jnp.int32, (8, LANES), 1)
    m = jnp.where(lane // (LANES // (2 * STEP)) == row, m, 0.0)
    return jnp.sum(m, axis=0, keepdims=True)


def two_hops(j, m, v0, v1, v2, links):
    hop(v0, v1, 4, 0, links)
    hop(v1, v2, 2, 1, links)
    m = set_row(m, j, own_norm(v1, 1))
    return set_row(m, j + 1, own_norm(v2, 0)) if j + 1 < 2 * STEP else m


def put_ahead(ahead, v2):
    for k in range(6):
        for x in range(2):
            ahead[2 * k + x] = v2[k, x]


def first_hops_kernel(own, low, high, ahead, moments, lx, ly, lz, lt, ltb, kept, *scratch):
    links = (lx, ly, lz, lt, ltb)
    v0, v1, v2 = scratch[:3]

    def side(msg, i, half):
        def at(k):
            c = 4 * (k % 2)
            return msg[i + k], msg[half + k // 2, slice(c, c + 4)]

        return at

    def store(dst, pieces):
        dst[0:8] = pieces[0]
        from_rim(dst, pieces[1])
        dst[10:14] = jnp.zeros((4, LANES), F32)

    behind, behind2, ahead1 = side(low, 0, 102), side(low, 72, 138), side(high, 0, 84)
    for k in range(18):
        store(lx.at[k, 0], behind2(k))
        store(lx.at[k, 1], behind(k))
        lx[k, 2] = own[k, 0]
        lx[k, 3] = own[k, 1]
        store(lx.at[k, 4], ahead1(k))
        for i, ref in ((36, lz), (54, lt)):
            store(ref.at[k, 0], behind(i + k))
            ref[k, 1] = own[i + k, 0]
            ref[k, 2] = own[i + k, 1]
            store(ref.at[k, 3], ahead1(i + k))
        for i in range(4):
            ltb[k, i] = pltpu.roll(lt[k, i], 1, 0)
        store(ly.at[k, 0], behind(18 + k))
        ly[k, 1] = own[18 + k, 0]
        ly[k, 2] = own[18 + k, 1]
        store(ly.at[k, 3], ahead1(18 + k))
    for i in range(4):
        for r in range(3):
            for c in range(r + 1):
                k, a = 3 * r + c, 3 * c + r
                u, w = ly[k, i], ly[a, i]
                ur, wr = pltpu.roll(u, NZ, 1), pltpu.roll(w, NZ, 1)
                ly[k, i] = u - wr
                if a != k:
                    ly[a, i] = w - ur
                u, w = ly[9 + k, i], ly[9 + a, i]
                ur, wr = pltpu.roll(u, NZ, 1), pltpu.roll(w, NZ, 1)
                ly[9 + k, i] = u + wr
                if a != k:
                    ly[9 + a, i] = w + ur
    for k in range(6):
        for x in range(2):
            kept[2 * k + x] = own[72 + k, x, 0:8]
            rim(kept, 12 + k, x, own[72 + k, x])
    kept[18:30] = low[90:102]
    kept[30:36] = low[147:153]
    kept[36:48] = high[72:84]
    kept[48:54] = high[120:126]
    unpack_wide(v0, kept, 0, 18, 36)
    m = set_row(jnp.zeros((8, LANES), F32), 0, own_norm(v0, 2))
    moments[...] = two_hops(1, m, v0, v1, v2, links)
    put_ahead(ahead, v2)


def hops_kernel(j, kind, own, low, high, before, lx, ly, lz, lt, ltb, *rest):
    links = (lx, ly, lz, lt, ltb)
    outs, (v0, v1, v2) = rest[:-3], rest[-3:]
    for k in range(6):
        for x in range(2):
            for i, ref in ((0, low), (2, own), (4, high)):
                v0[k, i + x, 0:8] = ref[2 * k + x]
                if kind == "wide":
                    from_rim(v0.at[k, i + x], ref[12 + k, 4 * x : 4 * x + 4])
    m = before[...]
    if kind == "last":
        (moments,) = outs
        hop(v0.at[:, 1:5], v2, 2, 1, links)
        moments[...] = message_row(set_row(m, j, own_norm(v2, 0)))
        return
    m = two_hops(j, m, v0, v1, v2, links)
    field, moments = outs
    if kind == "wide":
        put_ahead(field, v2)
    else:
        for k in range(6):
            for x in range(2):
                c = slice(4 * x, 4 * x + 4)
                field[k, c] = v2[k, x, 2:6]
                if field.shape[0] == 12:
                    field[6 + k, c] = own[2 * k + x, 2:6]
    moments[...] = message_row(m) if j + 1 == 2 * STEP else m


def spread_kernel(own, other, out):
    row = jnp.broadcast_to(own[...] + other[...], (8, LANES))
    for i in range(out.shape[0]):
        out[i] = row


def start_copies(fields, held, sems):
    copies = [pltpu.make_async_copy(f, h, sems.at[i]) for i, (f, h) in enumerate(zip(fields, held))]
    for c in copies:
        c.start()
    return copies


def restart_kernel(mass, gathered, shifts, lx, ly, lz, lt, ltb, *refs):
    fields, (r0, ahead, moments, state), scratch = refs[:7], refs[7:11], refs[11:]
    held, (sems, sum_, v0, v1, v2) = scratch[:7], scratch[7:]
    copies = start_copies(fields, held, sems)
    one = jnp.ones((8, LANES), F32)
    m = jnp.full((8, LANES), mass[0], F32)
    m2 = Pair(m * m, jnp.zeros_like(one))
    powers = summed_moments(gathered[...])
    s = first_state(powers, m2, shifts[...])
    leaves, _ = jax.tree_util.tree_flatten((s, [p.h for p in powers[:STEP]]))
    for i, leaf in enumerate(leaves):
        state[i : i + 1] = leaf[0:1]
    rest, top = s["handover"]
    c = [rest[0], -rest[1], rest[2], -rest[3], top]
    for copy in copies:
        copy.wait()
    kept, four, eight = held[0], held[1:4], held[4:7]
    for side in range(3):
        a, b, o = four[side], eight[side], 18 * side

        def one_tile(i, _, a=a, b=b, o=o):
            sum_[o + i] = (
                c[0] * kept[o + i]
                + c[1] * a[18 + i]
                + c[2] * a[i]
                + c[3] * b[18 + i]
                + c[4] * b[i]
            )
            return 0

        lax.fori_loop(0, 18, one_tile, 0)
    unpack_wide(v0, sum_, 0, 18, 36)
    for k in range(6):
        for x in range(2):
            r0[k, 4 * x : 4 * x + 4] = v0[k, 2 + x, 2:6]
    m = set_row(jnp.zeros((8, LANES), F32), 0, own_norm(v0, 2))
    moments[...] = two_hops(1, m, v0, v1, v2, (lx, ly, lz, lt, ltb))
    put_ahead(ahead, v2)


def finish_kernel(tree, mass, gathered, shifts, residues, state, *refs):
    fields, (out, act), scratch = refs[:7], refs[7:9], refs[9:]
    held, sems = scratch[:7], scratch[7]
    copies = start_copies(fields, held, sems)
    one = jnp.ones((8, LANES), F32)
    m = jnp.full((8, LANES), mass[0], F32)
    m2 = Pair(m * m, jnp.zeros_like(one))
    leaves = [jnp.broadcast_to(state[i : i + 1], (8, LANES)) for i in range(tree.num_leaves)]
    s, powers = jax.tree_util.tree_unflatten(tree, leaves)
    s = run_steps(STEP, summed_moments(gathered[...]), s, m2, one, shifts[...], True)
    weights = residues[...]
    c = [
        jnp.broadcast_to(jnp.sum(weights * s["sol"][j], axis=1, keepdims=True), (8, LANES))
        for j in range(2 * STEP)
    ]
    t = None
    for j in range(STEP):
        t = plus(t, c[j] * powers[j])
    act[...] = t
    c = [(v if j % 2 == 0 else -v)[0:4] for j, v in enumerate(c)]
    for copy in copies:
        copy.wait()
    start, four, eight, r0, r2, r4, r6 = held
    for k in range(6):
        for x in range(2):
            q, i = slice(4 * x, 4 * x + 4), 2 * k + x
            terms = (
                start[k, q],
                four[18 + i, 2:6],
                four[i, 2:6],
                eight[18 + i, 2:6],
                r0[k, q],
                r2[i, 2:6],
                r4[k, q],
                r6[i, 2:6],
            )
            t = None
            for w, v in zip(c, terms):
                t = plus(t, w * v)
            out[k, q] = t


def both_ways(x_up, x_down, axis):
    n = lax.axis_size(axis)
    up = [(i, (i + 1) % n) for i in range(n)]
    return lax.ppermute(x_up, axis, up), lax.ppermute(x_down, axis, [(b, a) for a, b in up])


def across(x, step):
    n = lax.axis_size(ZT)
    pairs = [
        (g * n + i, (1 - g) * n + (i + step) % n) for g in range(2) for i in range(n)
    ]
    return lax.ppermute(x, ("grp",) + ZT, pairs)


def everyone(row, later):
    n = lax.axis_size(REDUCE)
    tiles = -(-n // 8)
    other = lax.ppermute(row, "xy_1", [(0, 1), (1, 0)])
    (rows,) = call(spread_kernel, [(tiles, 8, LANES)], (row, other))
    rows = rows.reshape(8 * tiles, 1, LANES)[:n]
    rows, later = lax.optimization_barrier((rows, later))
    rows = lax.all_to_all(rows, REDUCE, 0, 0, tiled=True).reshape(n, LANES)
    return jnp.pad(rows, ((0, -n % 8), (0, 0))), later


def field_scratch(wide=True):
    tall = ROWS if wide else 8
    return [pltpu.VMEM((6, n, t, LANES), F32) for n, t in ((6, tall), (4, tall), (2, 8))]


def held_scratch(fields):
    return [pltpu.VMEM(f.shape, F32) for f in fields] + [pltpu.SemaphoreType.DMA((len(fields),))]


def state_shape():
    s = jax.ShapeDtypeStruct((8, LANES), F32)
    moments = [Pair(s, s)] * (2 * STEP)
    out = jax.eval_shape(first_state, moments, Pair(s, s), s)
    return jax.tree_util.tree_flatten((out, [s] * STEP))


def on_device(source, links, shifts, residues, mass):
    grp = lax.axis_index("grp")
    place, n_t = lax.axis_index(ZT), lax.axis_size(ZT)
    edges = [(place - 1) % n_t, place, (place + 1) % n_t]
    where = jnp.stack([grp] + [(e == n_t - 1).astype(jnp.int32) for e in edges])
    lane_shifts = jnp.broadcast_to(
        jnp.pad(shifts, (0, LANES - shifts.shape[0]), constant_values=1.0), (8, LANES)
    )
    mine = links.reshape(36, 8, LANES)
    start = source.reshape(LOCAL)
    both = jnp.concatenate([mine, start])
    low, high = both_ways(both, both, ZT)
    wide, up, down = call(
        wide_links_kernel,
        [(78, 2, ROWS, LANES), (UP_N, 8, LANES), (DOWN_N, 8, LANES)],
        (where, both, low, high, across(mine, 0), across(mine, 1), across(mine, -1)),
        1,
    )
    low, high = both_ways(up, down, XY)
    ahead_shape, row8, row1 = (12, 8, LANES), (8, LANES), (1, LANES)
    ahead, m, *rest = call(
        first_hops_kernel,
        [ahead_shape, row8, (18, 5, ROWS, LANES)]
        + [(18, 4, ROWS, LANES)] * 4
        + [(54, 8, LANES)],
        (wide, low, high),
        scratch=field_scratch(),
    )
    w, kept = rest[:5], rest[5]

    def hops(own, low, high, m, j, kind, fields=1):
        outs = {
            "wide": [ahead_shape, row8],
            "next": [(6 * fields, 8, LANES), row1 if j + 1 == 2 * STEP else row8],
            "last": [row1],
        }[kind]
        body = functools.partial(hops_kernel, j, kind)
        scratch = field_scratch(kind == "wide")
        return call(body, outs, (own, low, high, m, *w), scratch=scratch)

    def around(field):
        return (field, *both_ways(field, field, XY))

    def tall(field, low, high):
        shape = (3 * field.shape[0], 8, LANES)
        return call(wide_field_kernel, [shape], (field, low, high))[0]

    def taller(field):
        return tall(field, *both_ways(field, field, ZT))

    f4, m = hops(*around(ahead), m, 3, "next", 2)
    four = around(taller(f4))
    ahead, m = hops(*four, m, 5, "wide")
    f8, row = hops(*around(ahead), m, 7, "next", 2)
    gathered, f8 = everyone(row, f8)
    low, high = both_ways(f8, f8, ZT)
    eight = around(tall(f8, low, high))
    leaves, tree = state_shape()
    count = -(-len(leaves) // 8) * 8
    fields = (kept, *four, *eight)
    r0, r2, m, state = call(
        restart_kernel,
        [LOCAL, ahead_shape, row8, (count, LANES)],
        (mass, gathered, lane_shifts, *w, *fields),
        1,
        len(fields),
        held_scratch(fields) + [pltpu.VMEM((54, 8, LANES), F32)] + field_scratch(),
    )
    r4, m = hops(*around(r2), m, 3, "next")
    r6, m = hops(*around(taller(r4)), m, 5, "wide")
    (row,) = hops(*around(r6), m, 7, "last")
    lane_residues = jnp.broadcast_to(
        jnp.pad(residues, (0, LANES - residues.shape[0])), (8, LANES)
    )
    gathered, lane_residues = everyone(row, lane_residues)
    fields = (start, four[0], eight[0], r0, r2, r4, r6)
    rational, act = call(
        functools.partial(finish_kernel, tree),
        [LOCAL, row8],
        (mass, gathered, lane_shifts, lane_residues, state, *fields),
        1,
        len(fields),
        held_scratch(fields),
    )
    act = act[0:1]
    total = act + lax.ppermute(act, "grp", [(0, 1), (1, 0)])
    sites = source.shape[3] * lax.axis_size(XY) * source.shape[4] * n_t * LANES
    sites *= source.shape[0] * lax.axis_size("grp")
    return (rational.reshape(source.shape), (total / sites)[0, 0:1])


def solution(mesh):
    if mesh.size == 512:
        shape = (mesh.shape["grp"], 4, 4, 8, 2)
    else:
        shape = (mesh.shape["grp"], mesh.shape["zt"], 1, mesh.shape["xy"] // 2, 2)
    torus = Mesh(mesh.devices.reshape(shape), ("grp", "zt_0", "zt_1", "xy_0", "xy_1"))
    placed = (
        P("grp", None, None, XY, ZT, None),
        P("grp", None, None, None, XY, ZT, None),
        P(),
        P(),
        P(),
    )
    step = jax.shard_map(
        on_device,
        mesh=torus,
        in_specs=placed,
        out_specs=(P("grp", None, None, XY, ZT, None), P()),
        check_vma=False,
    )
    if mesh.size != 512:
        return step
    return step
```
